16 devices in a mesh: dp: 2 (over y, z), sp: 8 (over x, core).
Axes of the slice: x: 4, y: 2, z: 1, core: 2. Of those that a mesh axis runs over, the one named last changes fastest.
The devices are a block of a 4x4x8 slice.
Arguments:
- x: bfloat16 [16384, 2048], P(('dp', 'sp')), parts along dimension 0
- gain: bfloat16 [2048], replicated
- wq: bfloat16 [2048, 2048], P('sp')
- wk: bfloat16 [2048, 2048], P('sp')
- wv: bfloat16 [2048, 2048], P('sp')
- wo: bfloat16 [2048, 2048], P('sp')
Outputs:
- output: bfloat16 [16384, 2048], P(('dp', 'sp')), parts along dimension 0
There are 2 independent parts. The reference program is written for one: setup_inputs(seed, part) draws one part's arguments, and reference() takes and returns one part's arrays. A program takes and returns all parts, laid end to end along the dimension named above; an argument that names none is the same for every part.
All inputs are finite; a program needn't handle non-finite values.
Results may differ from the reference program's by a relative error of at most 0.012.
Values are sent between devices in bfloat16 or wider.
A program may use at most 768 MiB of HBM per device.

```python
import jax
import jax.numpy as jnp
from jax import lax

ROWS = 8192
D = 2048
HEADS = 8
KV_HEADS = 8
HEAD = 256
THETA = 10000


def setup_inputs(seed: int = 0, part: int = 0) -> dict:
    kx, kn, kq, kk, kv, ko = jax.random.split(jax.random.key(seed), 6)

    def weights(key, rows, columns):
        return jax.random.normal(key, (rows, columns), jnp.float32) * rows**-0.5

    drawn = {
        "x": jax.random.normal(jax.random.fold_in(kx, part), (ROWS, D), jnp.float32),
        "gain": 1 + 0.1 * jax.random.normal(kn, (D,), jnp.float32),
        "wq": 2 * weights(kq, D, HEADS * HEAD),
        "wk": 2 * weights(kk, D, KV_HEADS * HEAD),
        "wv": 4 * weights(kv, D, KV_HEADS * HEAD),
        "wo": weights(ko, HEADS * HEAD, D),
    }
    return {k: v.astype(jnp.bfloat16) for k, v in drawn.items()}


def normed(x, gain):
    wide = x.astype(jnp.float32)
    scale = lax.rsqrt(jnp.mean(wide * wide, -1, keepdims=True) + 1e-6)
    return (wide * scale * gain.astype(jnp.float32)).astype(jnp.bfloat16)


def turned(t, place, theta):
    half = t.shape[-1] // 2
    angle = place.astype(jnp.float32)[:, None] * theta ** (-jnp.arange(half, dtype=jnp.float32) / half)
    cos, sin = jnp.cos(angle)[:, None], jnp.sin(angle)[:, None]
    a, b = t[..., :half].astype(jnp.float32), t[..., half:].astype(jnp.float32)
    return jnp.concatenate([a * cos - b * sin, b * cos + a * sin], -1).astype(jnp.bfloat16)


def matmul(a, w):
    return jnp.dot(a, w, preferred_element_type=jnp.float32).astype(jnp.bfloat16)


def einsum(form, a, b):
    return jnp.einsum(form, a.astype(jnp.float32), b.astype(jnp.float32))


def attention(q, k, v):
    scores = einsum("tgsd,ugd->gstu", q, k) * q.shape[-1] ** -0.5
    token = jnp.arange(q.shape[0])
    scores = jnp.where(token[:, None] >= token, scores, -jnp.inf)
    weights = jax.nn.softmax(scores, -1).astype(jnp.bfloat16)
    return einsum("gstu,ugd->tgsd", weights, v).astype(jnp.bfloat16)


def reference(x, gain, wq, wk, wv, wo):
    a, place = normed(x, gain), jnp.arange(ROWS)
    q = turned(matmul(a, wq).reshape(ROWS, HEADS, HEAD), place, THETA).reshape(ROWS, KV_HEADS, -1, HEAD)
    k = turned(matmul(a, wk).reshape(ROWS, KV_HEADS, HEAD), place, THETA)
    v = matmul(a, wv).reshape(ROWS, KV_HEADS, HEAD)
    seen = attention(q, k, v).reshape(ROWS, HEADS * HEAD)
    return (x.astype(jnp.float32) + jnp.dot(seen, wo, preferred_element_type=jnp.float32)).astype(jnp.bfloat16)
```

```python
import functools

import jax
import jax.numpy as jnp
from jax import lax
from jax.experimental import pallas as pl
from jax.experimental.pallas import tpu as pltpu
from jax.sharding import PartitionSpec as P

MESH = pl.DeviceIdType.MESH
HEAD = 256
THETA = 10000
PIECE = 256
BLOCK = 512
STRIP = 256
HIDDEN = -2e30
LOG2E = 1.4426950408889634
VMEM = 62 * 2**20


def normed(x, gain):
    wide = x.astype(jnp.float32)
    scale = lax.rsqrt(jnp.mean(wide * wide, -1, keepdims=True) + 1e-6)
    return (wide * scale * gain.astype(jnp.float32)).astype(jnp.bfloat16)


def dot(a, b, ca, cb):
    return lax.dot_general(a, b, (((ca,), (cb,)), ((), ())), preferred_element_type=jnp.float32)


def kernel(n, a_ref, cosr, sinr, cosp, sinp, wq, wk, wv, wo, o_all, wo_all, a_all,
           w_s, stage, q_s, k_s, v_s, mix_s, top_s, s0, s1, o_s,
           send_w, recv_w, own_w, send_a, recv_a, load_s, send_r, send_o, recv_o, own_o, send_wo, recv_wo, own_wo):
    s = lax.axis_index("sp")
    core, chip = lax.rem(s, 2), lax.div(s, 2)
    chips = n // 2
    sib = s + 1 - 2 * core
    right, left = lax.rem(s + 2, n), lax.rem(s + n - 2, n)
    per = a_ref.shape[0] // PIECE
    e = HEAD**-0.5 * LOG2E

    def remote(src, dst, ss, rs, to):
        return pltpu.make_async_remote_copy(src_ref=src, dst_ref=dst, send_sem=ss, recv_sem=rs, device_id={"sp": to}, device_id_type=MESH)

    barrier = pltpu.get_barrier_semaphore()
    for off in range(1, n):
        pl.semaphore_signal(barrier, inc=1, device_id={"sp": lax.rem(s + off, n)}, device_id_type=MESH)
    pl.semaphore_wait(barrier, n - 1)

    def weight(i, m, to, frm):
        w = (wq, wk, wv)[m]
        depth = w.shape[0]
        return remote(w.at[:, pl.ds(pl.multiple_of(to * HEAD, HEAD), HEAD)],
                      w_s.at[pl.ds(pl.multiple_of(frm * depth, depth), depth), pl.ds(m * HEAD, HEAD)],
                      send_w.at[i, m], recv_w.at[i, m], to)

    def piece_of(i):
        return a_ref.at[pl.ds(pl.multiple_of(i * PIECE, PIECE), PIECE)]

    def swap(i):
        return remote(piece_of(i), a_all.at[per * s + i], send_a.at[i], recv_a.at[per * s + i], sib)

    for i in (0, 2, 1, 3):
        swap(i).start()
    for off in (4, 3, 5, 2, 6, 7, 1):
        for m in range(3):
            weight(off, m, lax.rem(s + off, n), s).start()
    own_weights = [pltpu.make_async_copy(w.at[:, pl.ds(pl.multiple_of(s * HEAD, HEAD), HEAD)],
                                         w_s.at[pl.ds(pl.multiple_of(s * w.shape[0], w.shape[0]), w.shape[0]), pl.ds(m * HEAD, HEAD)],
                                         own_w.at[m]) for m, w in enumerate((wq, wk, wv))]
    for c in own_weights:
        c.start()
    own_out = pltpu.make_async_copy(wo, wo_all.at[s], own_wo)
    own_out.start()

    def load_own(i, slot):
        return pltpu.make_async_copy(piece_of(i), stage.at[slot], load_s.at[slot])

    def load(g, slot):
        return pltpu.make_async_copy(a_all.at[g], stage.at[slot], load_s.at[slot])

    def arrived(g):
        return pltpu.make_async_remote_copy(src_ref=a_all.at[g], dst_ref=a_all.at[g], send_sem=send_a.at[0], recv_sem=recv_a.at[g],
                                            device_id={"sp": sib}, device_id_type=MESH).wait_recv()

    for i in range(per):
        load_own(i, i).start()

    for b in range(2):
        arrived(per * sib + 2 * b + core)

    def ring(i, b, to):
        g = 2 * per * chip + 2 * b + core
        mine = core == b // 2

        @pl.when(mine)
        def _():
            remote(piece_of(2 * (b % 2) + core), a_all.at[g], send_r.at[i], recv_a.at[g], to).start()

        @pl.when(jnp.logical_not(mine))
        def _():
            remote(a_all.at[g], a_all.at[g], send_r.at[i], recv_a.at[g], to).start()

    for i in range(4):
        ring(i, i, right)
        ring(4 + i, (i + 2) % 4, left)

    v_s[:, HEAD:, :] = jnp.ones_like(v_s[:, HEAD:, :])

    for c in own_weights:
        c.wait()
    for off in range(1, n):
        for m in range(3):
            weight(n - off, m, s, lax.rem(s + off, n)).wait_recv()

    def project(g, slot):
        y = dot(stage[slot], w_s[...], 1, 0)
        cp, sp = cosp[pl.ds(g, 1), :], sinp[pl.ds(g, 1), :]
        cr, sr = cosr[...], sinr[...]
        cos, sin = cp * cr - sp * sr, sp * cr + cp * sr
        b, at = lax.div(g, 2), pl.multiple_of(lax.rem(g, 2) * PIECE, PIECE)
        for ref, first in ((q_s, 0), (k_s, HEAD)):
            t = y[:, first : first + HEAD].astype(jnp.bfloat16).astype(jnp.float32)
            lo, hi = t[:, : HEAD // 2], t[:, HEAD // 2 :]
            ref[b, pl.ds(at, PIECE), :] = jnp.concatenate([lo * cos - hi * sin, hi * cos + lo * sin], -1).astype(jnp.bfloat16)
        v_s[b, :HEAD, pl.ds(at, PIECE)] = y[:, 2 * HEAD :].astype(jnp.bfloat16).T

    def diagonal(g):
        for h in range(BLOCK // STRIP):
            seen, cols = (h + 1) * STRIP, slice(h * STRIP, (h + 1) * STRIP)
            t = dot(k_s[g, :seen, :], q_s[g, cols, :], 1, 1)
            ok = lax.broadcasted_iota(jnp.int32, t.shape, 1) + h * STRIP >= lax.broadcasted_iota(jnp.int32, t.shape, 0)
            t = jnp.where(ok, t, HIDDEN)
            top = t.max(axis=0, keepdims=True)
            top_s[g, :, cols] = top
            mix_s[g, :, cols] = dot(v_s[g, :, :seen], jnp.exp2((t - top) * e).astype(jnp.bfloat16), 1, 0)

    def scores(pair):
        return dot(k_s[pair[1]], q_s[pair[0]], 1, 1)

    def pair_step(now, later, pair, following):
        later[...] = scores(following)
        q, k = pair
        values = v_s[k]
        for h in range(BLOCK // STRIP):
            cols = slice(h * STRIP, (h + 1) * STRIP)
            t = now[:, cols]
            old = top_s[q, :, cols]
            top = jnp.maximum(old, t.max(axis=0, keepdims=True))
            top_s[q, :, cols] = top
            p = jnp.exp2((t - top) * e).astype(jnp.bfloat16)
            mix_s[q, :, cols] = mix_s[q, :, cols] * jnp.exp2((old - top) * e) + dot(values, p, 1, 0)

    def pairs(count, pick):
        s0[...] = scores(pick(jnp.int32(0)))

        def body(u, _):
            t = 2 * u
            pair_step(s0, s1, pick(t), pick(jnp.minimum(t + 1, count - 1)))

            @pl.when(t + 1 < count)
            def _():
                pair_step(s1, s0, pick(t + 1), pick(jnp.minimum(t + 2, count - 1)))

        lax.fori_loop(0, lax.div(count + 1, 2), body, None)

    first = 4 * chip

    for i in range(per):
        load_own(i, i).wait()
    lax.fori_loop(0, per, lambda i, _: project(per * s + i, i), None)
    for b in range(2):
        arrived(per * sib + 2 * b + 1 - core)
    for i in range(per):
        load(per * sib + i, per + i).start()
    for i in range(per):
        load(per * sib + i, per + i).wait()
    lax.fori_loop(0, per, lambda i, _: project(per * sib + i, per + i), None)
    lax.fori_loop(0, 4, lambda b, _: diagonal(first + b), None)

    def pick_own(t):
        q = 1 + (t >= 1).astype(jnp.int32) + (t >= 3).astype(jnp.int32)
        return first + q, first + t - lax.div(q * (q - 1), 2)

    pairs(jnp.int32(6), pick_own)

    def place(r, side):
        far = (r > 4).astype(jnp.int32)
        away = lax.rem(jnp.where(side == 0, chips - 1 - far, 1 + far) + chip, chips)
        return 4 * away + lax.rem(r + jnp.where(side == 0, 3, 1), 4)

    def old(i):
        return jnp.where(i < 4, first + i, place(lax.div(i - 2, 2), lax.rem(i, 2)))

    def forward(i, g, to):
        return remote(a_all.at[g], a_all.at[g], send_r.at[i], recv_a.at[g], to)

    def relay(i, g):
        return remote(a_all.at[g], a_all.at[g], send_a.at[i], recv_a.at[g], sib)

    def turn(r, _):
        blocks = place(r, 0), place(r, 1)
        slot = 4 * lax.rem(r, 2)
        for i, b in enumerate(blocks):
            g = 2 * b + core
            arrived(g)
            relay(2 + 2 * r + i, g).start()

            @pl.when(r <= 2)
            def _():
                forward(8 + 2 * (r - 1) + i, g, (right, left)[i]).start()

            load(g, slot + i).start()

        for i, b in enumerate(blocks):
            load(2 * b + core, slot + i).wait()

        def half(i, _):
            project(2 * jnp.where(i == 0, blocks[0], blocks[1]) + core, slot + i)

        lax.fori_loop(0, 2, half, None)
        for i, b in enumerate(blocks):
            g = 2 * b + 1 - core
            arrived(g)
            load(g, slot + 2 + i).start()
        for i, b in enumerate(blocks):
            load(2 * b + 1 - core, slot + 2 + i).wait()

        def other(i, _):
            project(2 * jnp.where(i == 0, blocks[0], blocks[1]) + 1 - core, slot + 2 + i)

        lax.fori_loop(0, 2, other, None)
        lax.fori_loop(0, 2, lambda i, _: diagonal(jnp.where(i == 0, blocks[0], blocks[1])), None)

        def pick(t):
            new = jnp.where(lax.rem(t, 2) == 0, blocks[1], blocks[0])
            was = old(lax.div(t, 2))
            return jnp.maximum(new, was), jnp.minimum(new, was)

        pairs(5 + 4 * r, pick)

        @pl.when(r == 2)
        def _():
            for i, to in enumerate((right, left, sib)):
                remote(wo, wo_all.at[s], send_wo.at[i], recv_wo.at[s], to).start()

    lax.fori_loop(1, 7, turn, None)

    def came(d):
        return remote(wo_all.at[d], wo_all.at[d], send_wo.at[0], recv_wo.at[d], sib).wait_recv()

    def pass_on(i, d, to):
        return remote(wo_all.at[d], wo_all.at[d], send_wo.at[i], recv_wo.at[d], to)

    came(left)
    pass_on(3, left, sib).start()
    came(right)
    pass_on(4, right, sib).start()

    @pl.when(core == 0)
    def _():
        pass_on(5, left, right).start()

    @pl.when(core == 1)
    def _():
        pass_on(5, right, left).start()

    per_device = a_ref.shape[0] // BLOCK
    blocks = n * per_device

    def target(frm, b):
        return o_all.at[pl.ds(pl.multiple_of(lax.rem(b, per_device) * BLOCK, BLOCK), BLOCK), pl.ds(pl.multiple_of(frm * HEAD, HEAD), HEAD)]

    def give(b):
        to = lax.div(b, per_device)
        return remote(o_s.at[b], target(s, b), send_o.at[b], recv_o.at[s, lax.rem(b, per_device)], to)

    def keep(b):
        return pltpu.make_async_copy(o_s.at[b], target(s, b), own_o.at[lax.rem(b, per_device)])

    def finish(i, _):
        b = lax.rem(per_device * (s + 1) + i, blocks)
        mix = mix_s[b]
        o_s[b] = (mix[:HEAD] * (1 / mix[HEAD : HEAD + 1])).T.astype(jnp.bfloat16)

        @pl.when(i < blocks - per_device)
        def _():
            give(b).start()

        @pl.when(i >= blocks - per_device)
        def _():
            keep(b).start()

    lax.fori_loop(0, blocks, finish, None)

    far = lax.rem(s + 4, n)
    mine = far
    came(mine)
    pass_on(6, mine, sib).start()
    for d in (sib, far + 1 - 2 * core, left + 1 - 2 * core, right + 1 - 2 * core):
        came(d)

    for b in range(per_device):
        keep(per_device * s + b).wait()
        for off in range(1, n):
            frm = lax.rem(s + off, n)
            remote(o_s.at[b], target(frm, jnp.int32(b)), send_o.at[0], recv_o.at[frm, b], frm).wait_recv()
    own_out.wait()

    for off in range(1, n):
        for m in range(3):
            weight(off, m, lax.rem(s + off, n), s).wait_send()
    for i in range(per):
        swap(i).wait_send()
    for i in range(12):
        forward(i, jnp.int32(0), right).wait_send()
    for i in range(4, 16):
        relay(i, jnp.int32(0)).wait_send()
    for i in range(7):
        pass_on(i, jnp.int32(0), sib).wait_send()

    def sent(i, _):
        b = lax.rem(per_device * (s + 1) + i, blocks)
        give(b).wait_send()

    lax.fori_loop(0, blocks - per_device, sent, None)


def attention(n, a, tables, wq, wk, wv, wo):
    own, width = a.shape
    pieces, blocks = n * own // PIECE, n * own // BLOCK
    anywhere, whole = pl.BlockSpec(memory_space=pl.ANY), pl.BlockSpec(memory_space=pltpu.VMEM)
    dma = pltpu.SemaphoreType.DMA
    bf, f32 = jnp.bfloat16, jnp.float32
    tokens = n * own
    o_all, wo_all, _ = pl.pallas_call(
        functools.partial(kernel, n),
        in_specs=[anywhere] + [whole] * 4 + [anywhere] * 4,
        out_specs=[anywhere] * 3,
        out_shape=[jax.ShapeDtypeStruct((own, n * HEAD), bf), jax.ShapeDtypeStruct((n, *wo.shape), bf),
                   jax.ShapeDtypeStruct((pieces, PIECE, width), bf)],
        scratch_shapes=[
            pltpu.VMEM((width, 3 * HEAD), bf),
            pltpu.VMEM((8, PIECE, width), bf),
            pltpu.VMEM((blocks, BLOCK, HEAD), bf),
            pltpu.VMEM((blocks, BLOCK, HEAD), bf),
            pltpu.VMEM((blocks, HEAD + 8, BLOCK), bf),
            pltpu.VMEM((blocks, HEAD + 8, BLOCK), f32),
            pltpu.VMEM((blocks, 1, BLOCK), f32),
            pltpu.VMEM((BLOCK, BLOCK), f32),
            pltpu.VMEM((BLOCK, BLOCK), f32),
            pltpu.VMEM((blocks, BLOCK, HEAD), bf),
            dma((n, 3)), dma((n, 3)), dma((3,)), dma((16,)), dma((pieces,)), dma((8,)), dma((12,)),
            dma((blocks,)), dma((n, own // BLOCK)), dma((own // BLOCK,)), dma((7,)), dma((n,)), dma,
        ],
        compiler_params=pltpu.CompilerParams(collective_id=0, has_side_effects=True, vmem_limit_bytes=VMEM),
        cost_estimate=pl.CostEstimate(flops=2 * tokens * width * 3 * HEAD + 2 * tokens * tokens * HEAD,
                                      bytes_accessed=2 * tokens * width * 2, transcendentals=tokens * tokens // 2),
    )(a, *tables, wq, wk, wv, wo)
    return o_all, wo_all


def tables(pieces):
    half = HEAD // 2
    speed = THETA ** (-jnp.arange(half, dtype=jnp.float32) / half)
    near = jnp.arange(PIECE, dtype=jnp.float32)[:, None] * speed
    far = (jnp.arange(pieces, dtype=jnp.float32) * PIECE)[:, None] * speed
    return jnp.cos(near), jnp.sin(near), jnp.cos(far), jnp.sin(far)


def solution(mesh):
    n = mesh.shape["sp"]

    def step(x, gain, wq, wk, wv, wo):
        a = normed(x, gain)
        o, w = attention(n, a, tables(n * x.shape[0] // PIECE), wq, wk, wv, wo)
        y = jnp.dot(o, w.reshape(-1, w.shape[-1]), preferred_element_type=jnp.float32)
        return (x.astype(jnp.float32) + y).astype(jnp.bfloat16)

    tokens, whole = P(("dp", "sp"), None), P("sp", None)
    return jax.shard_map(
        step,
        mesh=mesh,
        in_specs=(tokens, P(None), whole, whole, whole, whole),
        out_specs=tokens,
        check_vma=False,
    )
```

```python
import functools

import jax
import jax.numpy as jnp
import numpy as np
from jax import lax
from jax.experimental import pallas as pl
from jax.experimental.pallas import tpu as pltpu
from jax.sharding import PartitionSpec as P

MESH = pl.DeviceIdType.MESH
HEAD = 256
THETA = 10000
PIECE = 256
BLOCK = 512
STRIP = 256
HIDDEN = -2e30
LOG2E = 1.4426950408889634
VMEM = 62 * 2**20


def dot(a, b, ca, cb):
    return lax.dot_general(a, b, (((ca,), (cb,)), ((), ())), preferred_element_type=jnp.float32)


def kernel(n, x_ref, gain, cosr, sinr, cosp, sinp, wq, wk, wv, wo, y_ref, a_all,
           w_s, own_s, stage, q_s, k_s, v_s, mix_s, top_s, s0, s1, o_s, o_in, wo_s,
           send_w, recv_w, own_w, send_a, recv_a, recv_f, load_s, send_r, send_o, recv_o, own_o, send_wo, recv_wo, own_wo, out_s):
    s, group = lax.axis_index("sp"), lax.axis_index("dp")
    core, chip = lax.rem(s, 2), lax.div(s, 2)
    chips = n // 2
    sib = s + 1 - 2 * core
    right, left = lax.rem(s + 2, n), lax.rem(s + n - 2, n)
    side = lax.rem(group, 2)
    other = group + 1 - 2 * side
    per = x_ref.shape[0] // PIECE
    depth = wq.shape[0]
    half = depth // 2
    e = HEAD**-0.5 * LOG2E

    def remote(src, dst, ss, rs, to):
        return pltpu.make_async_remote_copy(src_ref=src, dst_ref=dst, send_sem=ss, recv_sem=rs, device_id={"sp": to}, device_id_type=MESH)

    def across(src, dst, ss, rs):
        return pltpu.make_async_remote_copy(src_ref=src, dst_ref=dst, send_sem=ss, recv_sem=rs, device_id={"dp": other}, device_id_type=MESH)

    def load_own(i):
        return pltpu.make_async_copy(x_ref.at[pl.ds(i * PIECE, PIECE)], own_s.at[i], load_s.at[i])

    for i in range(per):
        load_own(i).start()

    barrier = pltpu.get_barrier_semaphore()
    for off in range(1, n):
        pl.semaphore_signal(barrier, inc=1, device_id={"sp": lax.rem(s + off, n)}, device_id_type=MESH)
    pl.semaphore_signal(barrier, inc=1, device_id={"dp": other}, device_id_type=MESH)
    pl.semaphore_wait(barrier, n)

    def rows(d, h):
        return pl.ds(pl.multiple_of(d * depth + h * half, half), half)

    def weight(off, m, frm, to):
        w = (wq, wk, wv)[m]
        return remote(w.at[pl.ds(pl.multiple_of(side * half, half), half), pl.ds(pl.multiple_of(to * HEAD, HEAD), HEAD)],
                      w_s.at[rows(frm, side), pl.ds(m * HEAD, HEAD)], send_w.at[off, m], recv_w.at[off, m], to)

    def hand(off, m, frm, h):
        part = w_s.at[rows(frm, h), pl.ds(m * HEAD, HEAD)]
        return across(part, part, send_w.at[n + off, m], recv_w.at[n + off, m])

    def to_sib(m, frm, to):
        w = (wq, wk, wv)[m]
        return remote(w.at[:, pl.ds(pl.multiple_of(to * HEAD, HEAD), HEAD)],
                      w_s.at[pl.ds(pl.multiple_of(frm * depth, depth), depth), pl.ds(m * HEAD, HEAD)], send_w.at[0, m], recv_w.at[0, m], to)

    away = [2, 6, 4, 3, 7, 5]

    def partner(off, back):
        base = lax.rem(s + (n - (off - off % 2) if back else off - off % 2), n)
        return base + 1 - 2 * core if off % 2 else base

    for off in away:
        for m in range(3):
            weight(off, m, s, partner(off, False)).start()
    for m in range(3):
        to_sib(m, s, sib).start()
    own_weights = [pltpu.make_async_copy(w.at[:, pl.ds(pl.multiple_of(s * HEAD, HEAD), HEAD)],
                                         w_s.at[pl.ds(pl.multiple_of(s * depth, depth), depth), pl.ds(m * HEAD, HEAD)],
                                         own_w.at[m]) for m, w in enumerate((wq, wk, wv))]
    for c in own_weights:
        c.start()
    own_out = pltpu.make_async_copy(wo, wo_s.at[pl.ds(pl.multiple_of(s * depth, depth), depth)], own_wo)
    own_out.start()

    def swap(i):
        return remote(own_s.at[i], a_all.at[per * s + i], send_a.at[i], recv_a.at[per * s + i], sib)

    def norm(i, rows_at_once=32):
        def some(j, _):
            at = pl.ds(pl.multiple_of(j * rows_at_once, rows_at_once), rows_at_once)
            wide = own_s[i, at, :].astype(jnp.float32)
            scale = lax.rsqrt(jnp.mean(wide * wide, -1, keepdims=True) + 1e-6)
            own_s[i, at, :] = (wide * scale * gain[...].astype(jnp.float32)).astype(jnp.bfloat16)

        lax.fori_loop(0, PIECE // rows_at_once, some, None)

    for i in range(per):
        load_own(i).wait()
        norm(i)
        if i:
            swap(i - 1).start()
    v_s[:, HEAD:, :] = jnp.ones_like(v_s[:, HEAD:, :])
    swap(per - 1).start()

    def load(g, slot):
        return pltpu.make_async_copy(a_all.at[g], stage.at[slot], load_s.at[slot])

    def arrived(g):
        remote(a_all.at[g], a_all.at[g], send_a.at[0], recv_a.at[g], sib).wait_recv()

    for b in range(2):
        arrived(per * sib + 2 * b + core)

    def ring(i, b, to):
        g = 2 * per * chip + 2 * b + core
        mine = core == b // 2

        @pl.when(mine)
        def _():
            remote(own_s.at[2 * (b % 2) + core], a_all.at[g], send_r.at[i], recv_a.at[g], to).start()

        @pl.when(jnp.logical_not(mine))
        def _():
            remote(a_all.at[g], a_all.at[g], send_r.at[i], recv_a.at[g], to).start()

    for i in range(4):
        ring(i, i, right)
        ring(4 + i, i, left)

    for off in away:
        frm = partner(off, True)
        for m in range(3):
            weight(off, m, frm, s).wait_recv()
            hand(off, m, frm, side).start()

    def project(piece, g):
        y = dot(piece, w_s[...], 1, 0)
        cp, sp = cosp[pl.ds(g, 1), :], sinp[pl.ds(g, 1), :]
        cr, sr = cosr[...], sinr[...]
        cos, sin = cp * cr - sp * sr, sp * cr + cp * sr
        b, at = lax.div(g, 2), pl.multiple_of(lax.rem(g, 2) * PIECE, PIECE)
        for ref, first in ((q_s, 0), (k_s, HEAD)):
            t = y[:, first : first + HEAD].astype(jnp.bfloat16).astype(jnp.float32)
            lo, hi = t[:, : HEAD // 2], t[:, HEAD // 2 :]
            ref[b, pl.ds(at, PIECE), :] = jnp.concatenate([lo * cos - hi * sin, hi * cos + lo * sin], -1).astype(jnp.bfloat16)
        v_s[b, :HEAD, pl.ds(at, PIECE)] = y[:, 2 * HEAD :].astype(jnp.bfloat16).T

    def diagonal(g):
        for h in range(BLOCK // STRIP):
            seen, cols = (h + 1) * STRIP, slice(h * STRIP, (h + 1) * STRIP)
            t = dot(k_s[g, :seen, :], q_s[g, cols, :], 1, 1)
            ok = lax.broadcasted_iota(jnp.int32, t.shape, 1) + h * STRIP >= lax.broadcasted_iota(jnp.int32, t.shape, 0)
            t = jnp.where(ok, t, HIDDEN)
            top = t.max(axis=0, keepdims=True)
            top_s[g, :, cols] = top
            mix_s[g, :, cols] = dot(v_s[g, :, :seen], jnp.exp2((t - top) * e).astype(jnp.bfloat16), 1, 0)

    def scores(pair):
        return dot(k_s[pair[1]], q_s[pair[0]], 1, 1)

    def pair_step(now, later, pair, following):
        later[...] = scores(following)
        q, k = pair
        values = v_s[k]
        for h in range(BLOCK // STRIP):
            cols = slice(h * STRIP, (h + 1) * STRIP)
            t = now[:, cols]
            old = top_s[q, :, cols]
            top = jnp.maximum(old, t.max(axis=0, keepdims=True))
            top_s[q, :, cols] = top
            p = jnp.exp2((t - top) * e).astype(jnp.bfloat16)
            mix_s[q, :, cols] = mix_s[q, :, cols] * jnp.exp2((old - top) * e) + dot(values, p, 1, 0)

    def pairs(count, pick):
        s0[...] = scores(pick(jnp.int32(0)))

        def body(u, _):
            t = 2 * u
            pair_step(s0, s1, pick(t), pick(jnp.minimum(t + 1, count - 1)))

            @pl.when(t + 1 < count)
            def _():
                pair_step(s1, s0, pick(t + 1), pick(jnp.minimum(t + 2, count - 1)))

        lax.fori_loop(0, lax.div(count + 1, 2), body, None)

    first = 4 * chip

    for b in range(2):
        arrived(per * sib + 2 * b + 1 - core)
    for i in range(per):
        load(per * sib + i, i).start()
    for c in own_weights:
        c.wait()
    for m in range(3):
        to_sib(m, sib, s).wait_recv()
    for off in away:
        for m in range(3):
            hand(off, m, partner(off, True), 1 - side).wait_recv()
    lax.fori_loop(0, per, lambda i, _: project(own_s[i], per * s + i), None)
    for i in range(per):
        load(per * sib + i, i).wait()
    lax.fori_loop(0, per, lambda i, _: project(stage[i], per * sib + i), None)
    lax.fori_loop(0, 4, lambda b, _: diagonal(first + b), None)

    def pick_own(t):
        q = 1 + (t >= 1).astype(jnp.int32) + (t >= 3).astype(jnp.int32)
        return first + q, first + t - lax.div(q * (q - 1), 2)

    pairs(jnp.int32(6), pick_own)

    chip_left, chip_right, chip_far = (4 * lax.rem(chip + d, chips) for d in (chips - 1, 1, 2))

    def old(i):
        near = jnp.where(lax.rem(i, 2) == 0, chip_left, chip_right) + lax.div(i - 4, 2)
        return jnp.where(i < 4, first + i, jnp.where(i < 12, near, chip_far + i - 12))

    def relay(i, g):
        return remote(a_all.at[g], a_all.at[g], send_a.at[i], recv_a.at[g], sib)

    def forward(i, g, h, to):
        part = a_all.at[g, pl.ds(h * (PIECE // 2), PIECE // 2)]
        return remote(part, part, send_r.at[i], recv_f.at[lax.rem(lax.div(g, 2), 4), h], to)

    def turn(r, _):
        blocks = chip_left + r - 1, chip_right + r - 1
        for i, b in enumerate(blocks):
            g = 2 * b + core
            arrived(g)
            relay(2 + 2 * r + i, g).start()
            forward(8 + 2 * (r - 1) + i, g, i, (right, left)[i]).start()
            load(g, i).start()

        def go(i, parity, slot):
            project(stage[slot], 2 * jnp.where(i == 0, blocks[0], blocks[1]) + parity)

        for i, b in enumerate(blocks):
            load(2 * b + core, i).wait()
        lax.fori_loop(0, 2, lambda i, _: go(i, core, i), None)
        for i, b in enumerate(blocks):
            g = 2 * b + 1 - core
            arrived(g)
            load(g, 2 + i).start()
        for i, b in enumerate(blocks):
            load(2 * b + 1 - core, 2 + i).wait()
        lax.fori_loop(0, 2, lambda i, _: go(i, 1 - core, 2 + i), None)
        lax.fori_loop(0, 2, lambda i, _: diagonal(jnp.where(i == 0, blocks[0], blocks[1])), None)

        def pick(t):
            new = jnp.where(lax.rem(t, 2) == 0, blocks[1], blocks[0])
            was = old(lax.div(t, 2))
            return jnp.maximum(new, was), jnp.minimum(new, was)

        pairs(5 + 4 * r, pick)

    lax.fori_loop(1, 5, turn, None)

    def out_rows(d, h):
        return wo_s.at[rows(d, h)]

    def out_own(i, h, to):
        return remote(wo.at[pl.ds(pl.multiple_of(h * half, half), half)], out_rows(s, h), send_wo.at[i], recv_wo.at[s, h], to)

    def came(d, h):
        remote(out_rows(d, h), out_rows(d, h), send_wo.at[0], recv_wo.at[d, h], sib).wait_recv()

    def pass_on(i, d, h, to):
        return remote(out_rows(d, h), out_rows(d, h), send_wo.at[i], recv_wo.at[d, h], to)

    def pass_across(i, d):
        return across(out_rows(d, side), out_rows(d, side), send_wo.at[i], recv_wo.at[d, side])

    out_own(0, side, right).start()
    out_own(1, side, left).start()
    out_own(2, jnp.int32(0), sib).start()
    out_own(3, jnp.int32(1), sib).start()

    def far_turn(r, _):
        b = chip_far + r
        g = 2 * b + core
        for h in range(2):
            forward(0, g, h, sib).wait_recv()
        relay(12 + r, g).start()
        load(g, 0).start()
        load(g, 0).wait()
        project(stage[0], g)
        g = 2 * b + 1 - core
        arrived(g)
        load(g, 1).start()
        load(g, 1).wait()
        project(stage[1], g)
        diagonal(b)

        def pick(t):
            was = old(t)
            return jnp.maximum(b, was), jnp.minimum(b, was)

        pairs(12 + r, pick)

    lax.fori_loop(0, 4, far_turn, None)

    far = lax.rem(s + 4, n)
    came(left, side)
    came(right, side)

    @pl.when(core == 0)
    def _():
        pass_on(4, left, side, right).start()

    @pl.when(core == 1)
    def _():
        pass_on(4, right, side, left).start()

    for i, d in enumerate((left, right)):
        pass_across(5 + i, d).start()
        pass_on(7 + i, d, side, sib).start()

    pieces = n * per

    def dest(i):
        return lax.rem(s + 1 + lax.rem(i, n), n), lax.div(i, n)

    def target(frm, part):
        return o_in.at[pl.ds(pl.multiple_of(part * PIECE, PIECE), PIECE), pl.ds(pl.multiple_of(frm * HEAD, HEAD), HEAD)]

    def give(i):
        to, part = dest(i)
        return remote(o_s.at[per * to + part], target(s, part), send_o.at[i], recv_o.at[s, part], to)

    def keep(part):
        return pltpu.make_async_copy(o_s.at[per * s + part], target(s, part), own_o.at[part])

    def send(i):
        @pl.when(lax.rem(i, n) < n - 1)
        def _():
            give(i).start()

        @pl.when(lax.rem(i, n) == n - 1)
        def _():
            keep(lax.div(i, n)).start()

    def finish(i, _):
        to, part = dest(i)
        g = per * to + part
        mix = mix_s[lax.div(g, 2), :, pl.ds(pl.multiple_of(lax.rem(g, 2) * PIECE, PIECE), PIECE)]
        o_s[g] = (mix[:HEAD] * (1 / mix[HEAD : HEAD + 1])).T.astype(jnp.bfloat16)

        @pl.when(i > 0)
        def _():
            send(i - 1)

    lax.fori_loop(0, pieces, finish, None)

    for i in range(per):
        swap(i).wait_send()
    for i in range(8):
        remote(own_s.at[0], own_s.at[0], send_r.at[i], recv_a.at[0], sib).wait_send()
    for i in range(per):
        load_own(i).start()
    send(jnp.int32(pieces - 1))

    came(far, side)
    pass_across(9, far).start()
    pass_on(10, far, side, sib).start()
    for i, d in enumerate((left, right, far)):
        came(d, 1 - side)
        pass_on(11 + i, d, 1 - side, sib).start()
    for h in range(2):
        came(sib, jnp.int32(h))
        for d in (left, right, far):
            came(d + 1 - 2 * core, jnp.int32(h))
    own_out.wait()
    for i in range(per):
        load_own(i).wait()

    wide = wo_s.shape[1] // 4

    def out(part):
        return pltpu.make_async_copy(stage.at[part], y_ref.at[pl.ds(pl.multiple_of(part * PIECE, PIECE), PIECE)], out_s.at[part])

    def last(part, _):
        keep(part).wait()
        for off in range(1, n):
            frm = lax.rem(s + off, n)
            remote(o_s.at[0], target(frm, part), send_o.at[0], recv_o.at[frm, part], frm).wait_recv()

        def columns(j, _):
            cols = pl.ds(pl.multiple_of(j * wide, wide), wide)
            y = dot(o_in[pl.ds(pl.multiple_of(part * PIECE, PIECE), PIECE), :], wo_s[:, cols], 1, 0)
            stage[part, :, cols] = (own_s[part, :, cols].astype(jnp.float32) + y).astype(jnp.bfloat16)

        lax.fori_loop(0, wo_s.shape[1] // wide, columns, None)
        out(part).start()

    lax.fori_loop(0, per, last, None)

    for off in away:
        for m in range(3):
            weight(off, m, s, partner(off, False)).wait_send()
            hand(off, m, partner(off, True), side).wait_send()
    for m in range(3):
        to_sib(m, s, sib).wait_send()
    for i in range(8):
        forward(8 + i, jnp.int32(0), 0, right).wait_send()
    for i in range(4, 16):
        relay(i, jnp.int32(0)).wait_send()
    for i in range(14):
        pass_on(i, jnp.int32(0), jnp.int32(0), sib).wait_send()

    def sent(i, _):
        @pl.when(lax.rem(i, n) < n - 1)
        def _():
            give(i).wait_send()

    lax.fori_loop(0, pieces, sent, None)
    for i in range(per):
        out(jnp.int32(i)).wait()


def layer(n, x, gain, tables, wq, wk, wv, wo):
    own, width = x.shape
    pieces, blocks = n * own // PIECE, n * own // BLOCK
    anywhere, whole = pl.BlockSpec(memory_space=pl.ANY), pl.BlockSpec(memory_space=pltpu.VMEM)
    dma = pltpu.SemaphoreType.DMA
    bf, f32 = jnp.bfloat16, jnp.float32
    tokens, per = n * own, own // PIECE
    y, _ = pl.pallas_call(
        functools.partial(kernel, n),
        in_specs=[anywhere] + [whole] * 5 + [anywhere] * 4,
        out_specs=[anywhere] * 2,
        out_shape=[jax.ShapeDtypeStruct(x.shape, bf), jax.ShapeDtypeStruct((pieces, PIECE, width), bf)],
        scratch_shapes=[
            pltpu.VMEM((width, 3 * HEAD), bf),
            pltpu.VMEM((per, PIECE, width), bf),
            pltpu.VMEM((4, PIECE, width), bf),
            pltpu.VMEM((blocks, BLOCK, HEAD), bf),
            pltpu.VMEM((blocks, BLOCK, HEAD), bf),
            pltpu.VMEM((blocks, HEAD + 8, BLOCK), bf),
            pltpu.VMEM((blocks, HEAD + 8, BLOCK), f32),
            pltpu.VMEM((blocks, 1, BLOCK), f32),
            pltpu.VMEM((BLOCK, BLOCK), f32),
            pltpu.VMEM((BLOCK, BLOCK), f32),
            pltpu.VMEM((pieces, PIECE, HEAD), bf),
            pltpu.VMEM((own, n * HEAD), bf),
            pltpu.VMEM((n * HEAD, width), bf),
            dma((2 * n, 3)), dma((2 * n, 3)), dma((3,)), dma((16,)), dma((pieces,)), dma((4, 2)), dma((4,)), dma((16,)),
            dma((pieces,)), dma((n, per)), dma((per,)), dma((14,)), dma((n, 2)), dma, dma((per,)),
        ],
        compiler_params=pltpu.CompilerParams(collective_id=0, has_side_effects=True, vmem_limit_bytes=VMEM),
        cost_estimate=pl.CostEstimate(flops=2 * tokens * width * 4 * HEAD + 2 * tokens * tokens * HEAD,
                                      bytes_accessed=2 * tokens * width * 2, transcendentals=tokens * tokens // 2),
    )(x, gain[None], *tables, wq, wk, wv, wo)
    return y


def tables(pieces):
    speed = float(THETA) ** (-np.arange(HEAD // 2) / (HEAD // 2))
    near, far = np.arange(PIECE)[:, None] * speed, (np.arange(pieces) * PIECE)[:, None] * speed
    return tuple(jnp.asarray(f(t), jnp.float32) for t in (near, far) for f in (np.cos, np.sin))


def solution(mesh):
    n = mesh.shape["sp"]

    def step(x, gain, wq, wk, wv, wo):
        return layer(n, x, gain, tables(n * x.shape[0] // PIECE), wq, wk, wv, wo)

    tokens, whole = P(("dp", "sp"), None), P("sp", None)
    return jax.shard_map(
        step,
        mesh=mesh,
        in_specs=(tokens, P(None), whole, whole, whole, whole),
        out_specs=tokens,
        check_vma=False,
    )
```

```python
import functools

import jax
import jax.numpy as jnp
import numpy as np
from jax import lax
from jax.experimental import pallas as pl
from jax.experimental.pallas import tpu as pltpu
from jax.sharding import PartitionSpec as P

MESH = pl.DeviceIdType.MESH
HEAD = 256
THETA = 10000
PIECE = 256
BLOCK = 512
STRIP = 256
NEAR = 128
HIDDEN = -2e30
LOG2E = 1.4426950408889634
VMEM = 67043328


def dot(a, b, ca, cb):
    return lax.dot_general(a, b, (((ca,), (cb,)), ((), ())), preferred_element_type=jnp.float32)


def kernel(n, x_ref, gain, cosr, sinr, cosp, sinp, wq, wk, wv, wo, y_ref, wo_all,
           w_s, own_s, land, q_s, k_s, v_s, mix_s, top_s, s0, s1, o_in,
           send_w, recv_w, own_w, send_a, recv_a, recv_f, load_s, send_r, send_o, recv_o, own_o, send_wo, recv_wo, own_wo, out_s):
    s, group = lax.axis_index("sp"), lax.axis_index("dp")
    core, chip = lax.rem(s, 2), lax.div(s, 2)
    chips = n // 2
    sib = s + 1 - 2 * core
    right, left = lax.rem(s + 2, n), lax.rem(s + n - 2, n)
    side = lax.rem(group, 2)
    other = group + 1 - 2 * side
    per = x_ref.shape[0] // PIECE
    depth = wq.shape[0]
    half = depth // 2
    e = HEAD**-0.5 * LOG2E

    def remote(src, dst, ss, rs, to):
        return pltpu.make_async_remote_copy(src_ref=src, dst_ref=dst, send_sem=ss, recv_sem=rs, device_id={"sp": to}, device_id_type=MESH)

    def across(src, dst, ss, rs):
        return pltpu.make_async_remote_copy(src_ref=src, dst_ref=dst, send_sem=ss, recv_sem=rs, device_id={"dp": other}, device_id_type=MESH)

    def load_own(i):
        return pltpu.make_async_copy(x_ref.at[pl.ds(i * PIECE, PIECE)], own_s.at[i], load_s.at[i])

    for i in range(per):
        load_own(i).start()

    barrier = pltpu.get_barrier_semaphore()
    for off in range(1, n):
        pl.semaphore_signal(barrier, inc=1, device_id={"sp": lax.rem(s + off, n)}, device_id_type=MESH)
    pl.semaphore_signal(barrier, inc=1, device_id={"dp": other}, device_id_type=MESH)
    pl.semaphore_wait(barrier, n)

    def rows(d, h):
        return pl.ds(pl.multiple_of(d * depth + h * half, half), half)

    def weight(off, m, frm, to):
        w = (wq, wk, wv)[m]
        return remote(w.at[pl.ds(pl.multiple_of(side * half, half), half), pl.ds(pl.multiple_of(to * HEAD, HEAD), HEAD)],
                      w_s.at[rows(frm, side), pl.ds(m * HEAD, HEAD)], send_w.at[off, m], recv_w.at[off, m], to)

    def hand(off, m, frm, h):
        part = w_s.at[rows(frm, h), pl.ds(m * HEAD, HEAD)]
        return across(part, part, send_w.at[n + off, m], recv_w.at[n + off, m])

    def to_sib(m, frm, to):
        w = (wq, wk, wv)[m]
        return remote(w.at[:, pl.ds(pl.multiple_of(to * HEAD, HEAD), HEAD)],
                      w_s.at[pl.ds(pl.multiple_of(frm * depth, depth), depth), pl.ds(m * HEAD, HEAD)], send_w.at[0, m], recv_w.at[0, m], to)

    away = [2, 6, 4, 3, 7, 5]

    def partner(off, back):
        base = lax.rem(s + (n - (off - off % 2) if back else off - off % 2), n)
        return base + 1 - 2 * core if off % 2 else base

    for off in away:
        for m in range(3):
            weight(off, m, s, partner(off, False)).start()
    for m in range(3):
        to_sib(m, s, sib).start()
    own_weights = [pltpu.make_async_copy(w.at[:, pl.ds(pl.multiple_of(s * HEAD, HEAD), HEAD)],
                                         w_s.at[pl.ds(pl.multiple_of(s * depth, depth), depth), pl.ds(m * HEAD, HEAD)],
                                         own_w.at[m]) for m, w in enumerate((wq, wk, wv))]
    for c in own_weights:
        c.start()
    own_out = pltpu.make_async_copy(wo, wo_all.at[pl.ds(pl.multiple_of(s * depth, depth), depth)], own_wo)
    own_out.start()

    def from_left(b, by):
        return 4 * b + by

    def from_right(b, by):
        return 4 * b + 2 + by

    def from_far(b, by):
        return 16 + 2 * b + by

    def from_sib(i):
        return 24 + i

    def swap(i):
        return remote(own_s.at[i], land.at[from_sib(i)], send_a.at[i], recv_a.at[from_sib(i)], sib)

    def norm(i, rows_at_once=32):
        def some(j, _):
            at = pl.ds(pl.multiple_of(j * rows_at_once, rows_at_once), rows_at_once)
            wide = own_s[i, at, :].astype(jnp.float32)
            scale = lax.rsqrt(jnp.mean(wide * wide, -1, keepdims=True) + 1e-6)
            own_s[i, at, :] = (wide * scale * gain[...].astype(jnp.float32)[None]).astype(jnp.bfloat16)

        lax.fori_loop(0, PIECE // rows_at_once, some, None)

    for i in range(per):
        load_own(i).wait()
        norm(i)
        if i:
            swap(i - 1).start()
    swap(per - 1).start()

    def arrived(slot):
        remote(land.at[slot], land.at[slot], send_a.at[0], recv_a.at[slot], sib).wait_recv()

    for b in range(2):
        arrived(from_sib(2 * b + core))

    def ring(i, b, to, slot):
        mine = core == b // 2

        @pl.when(mine)
        def _():
            remote(own_s.at[2 * (b % 2) + core], land.at[slot], send_r.at[i], recv_a.at[slot], to).start()

        @pl.when(jnp.logical_not(mine))
        def _():
            remote(land.at[from_sib(2 * (b % 2) + core)], land.at[slot], send_r.at[i], recv_a.at[slot], to).start()

    for b in range(4):
        ring(b, b, right, from_left(b, core))
        ring(4 + b, b, left, from_right(b, core))

    for off in away:
        frm = partner(off, True)
        for m in range(3):
            weight(off, m, frm, s).wait_recv()
            hand(off, m, frm, side).start()

    def project(piece, g):
        y = dot(piece, w_s[...], 1, 0)
        cr, sr, turns = cosr[...], sinr[...], []
        for h in range(PIECE // NEAR):
            at = pl.ds(g * (PIECE // NEAR) + h, 1)
            cp, sp = cosp[at, :], sinp[at, :]
            turns.append((cp * cr - sp * sr, sp * cr + cp * sr))
        cos, sin = (jnp.concatenate(t, 0) for t in zip(*turns))
        b, at = lax.div(g, 2), pl.multiple_of(lax.rem(g, 2) * PIECE, PIECE)
        for ref, first in ((q_s, 0), (k_s, HEAD)):
            t = y[:, first : first + HEAD].astype(jnp.bfloat16).astype(jnp.float32)
            lo, hi = t[:, : HEAD // 2], t[:, HEAD // 2 :]
            ref[b, pl.ds(at, PIECE), :] = jnp.concatenate([lo * cos - hi * sin, hi * cos + lo * sin], -1).astype(jnp.bfloat16)
        v_s[b, :, pl.ds(at, PIECE)] = y[:, 2 * HEAD :].astype(jnp.bfloat16).T

    def diagonal(g):
        for h in range(BLOCK // STRIP):
            seen, cols = (h + 1) * STRIP, slice(h * STRIP, (h + 1) * STRIP)
            t = dot(k_s[g, :seen, :], q_s[g, cols, :], 1, 1)
            ok = lax.broadcasted_iota(jnp.int32, t.shape, 1) + h * STRIP >= lax.broadcasted_iota(jnp.int32, t.shape, 0)
            t = jnp.where(ok, t, HIDDEN)
            top = t.max(axis=0, keepdims=True)
            top_s[pl.ds(g, 1), cols] = top
            values = jnp.concatenate([v_s[g, :, :seen], jnp.ones((8, seen), jnp.bfloat16)], 0)
            mix_s[g, :, cols] = dot(values, jnp.exp2((t - top) * e).astype(jnp.bfloat16), 1, 0)

    def scores(pair):
        return dot(k_s[pair[1]], q_s[pair[0]], 1, 1)

    def pair_step(now, later, pair, following):
        later[...] = scores(following)
        q, k = pair
        values = jnp.concatenate([v_s[k], jnp.ones((8, BLOCK), jnp.bfloat16)], 0)
        for h in range(BLOCK // STRIP):
            cols = slice(h * STRIP, (h + 1) * STRIP)
            t = now[:, cols]
            old = top_s[pl.ds(q, 1), cols]
            top = jnp.maximum(old, t.max(axis=0, keepdims=True))
            top_s[pl.ds(q, 1), cols] = top
            p = jnp.exp2((t - top) * e).astype(jnp.bfloat16)
            mix_s[q, :, cols] = mix_s[q, :, cols] * jnp.exp2((old - top) * e) + dot(values, p, 1, 0)

    def pairs(count, pick, meanwhile):
        s0[...] = scores(pick(jnp.int32(0)))
        turns = lax.div(count + 1, 2)

        def body(u, _):
            t = 2 * u

            @pl.when(u == jnp.maximum(turns - 3, 0))
            def _():
                meanwhile()

            pair_step(s0, s1, pick(t), pick(jnp.minimum(t + 1, count - 1)))

            @pl.when(t + 1 < count)
            def _():
                pair_step(s1, s0, pick(t + 1), pick(jnp.minimum(t + 2, count - 1)))

        lax.fori_loop(0, turns, body, None)

    first = 4 * chip
    chip_left, chip_right, chip_far = (4 * lax.rem(chip + d, chips) for d in (chips - 1, 1, 2))

    def old(i):
        near = jnp.where(lax.rem(i, 2) == 0, chip_left, chip_right) + lax.div(i - 4, 2)
        return jnp.where(i < 4, first + i, jnp.where(i < 12, near, chip_far + i - 12))

    def relay(i, slot):
        return remote(land.at[slot], land.at[slot], send_a.at[i], recv_a.at[slot], sib)

    def forward(i, slot, b, h, to):
        at = pl.ds(h * (PIECE // 2), PIECE // 2)
        return remote(land.at[slot, at], land.at[from_far(b, core), at], send_r.at[i], recv_f.at[b, h], to)

    def near_come(b):
        for i, slot in enumerate((from_left(b, core), from_right(b, core))):
            arrived(slot)
            relay(4 + 2 * b + i, slot).start()
            forward(8 + 2 * b + i, slot, b, i, (right, left)[i]).start()

    def far_come(b):
        for h in range(2):
            forward(0, jnp.int32(0), b, h, sib).wait_recv()
        relay(12 + b, from_far(b, core)).start()

    for c in own_weights:
        c.wait()
    for m in range(3):
        to_sib(m, sib, s).wait_recv()
    for off in away:
        for m in range(3):
            hand(off, m, partner(off, True), 1 - side).wait_recv()
    lax.fori_loop(0, per, lambda i, _: project(own_s[i], per * s + i), None)
    for b in range(2):
        arrived(from_sib(2 * b + 1 - core))
    lax.fori_loop(0, per, lambda i, _: project(land[from_sib(i)], per * sib + i), None)
    lax.fori_loop(0, 4, lambda b, _: diagonal(first + b), None)

    def pick_own(t):
        q = 1 + (t >= 1).astype(jnp.int32) + (t >= 3).astype(jnp.int32)
        return first + q, first + t - lax.div(q * (q - 1), 2)

    pairs(jnp.int32(6), pick_own, lambda: near_come(jnp.int32(0)))

    def turn(r, _):
        blocks = chip_left + r, chip_right + r

        def go(i, _):
            by = jnp.where(i < 2, core, 1 - core)

            @pl.when(i == 2)
            def _():
                arrived(from_left(r, 1 - core))
                arrived(from_right(r, 1 - core))

            even = lax.rem(i, 2) == 0
            project(land[jnp.where(even, from_left(r, by), from_right(r, by))], 2 * jnp.where(even, blocks[0], blocks[1]) + by)

        lax.fori_loop(0, 4, go, None)
        lax.fori_loop(0, 2, lambda i, _: diagonal(jnp.where(i == 0, blocks[0], blocks[1])), None)

        def pick(t):
            new = jnp.where(lax.rem(t, 2) == 0, blocks[1], blocks[0])
            was = old(lax.div(t, 2))
            return jnp.maximum(new, was), jnp.minimum(new, was)

        def meanwhile():
            @pl.when(r < 3)
            def _():
                near_come(r + 1)

            @pl.when(r == 3)
            def _():
                far_come(jnp.int32(0))

        pairs(9 + 4 * r, pick, meanwhile)

    lax.fori_loop(0, 4, turn, None)

    def out_rows(d, h):
        return wo_all.at[rows(d, h)]

    def out_own(i, h, to):
        return remote(wo.at[pl.ds(pl.multiple_of(h * half, half), half)], out_rows(s, h), send_wo.at[i], recv_wo.at[s, h], to)

    def came(d, h):
        remote(out_rows(d, h), out_rows(d, h), send_wo.at[0], recv_wo.at[d, h], sib).wait_recv()

    def pass_on(i, d, h, to):
        return remote(out_rows(d, h), out_rows(d, h), send_wo.at[i], recv_wo.at[d, h], to)

    def pass_across(i, d):
        return across(out_rows(d, side), out_rows(d, side), send_wo.at[i], recv_wo.at[d, side])

    out_own(0, side, right).start()
    out_own(1, side, left).start()
    out_own(2, jnp.int32(0), sib).start()
    out_own(3, jnp.int32(1), sib).start()

    def far_turn(r, _):
        b = chip_far + r

        def go(i, _):
            by = jnp.where(i == 0, core, 1 - core)

            @pl.when(i == 1)
            def _():
                arrived(from_far(r, 1 - core))

            project(land[from_far(r, by)], 2 * b + by)

        lax.fori_loop(0, 2, go, None)
        diagonal(b)

        def pick(t):
            was = old(t)
            return jnp.maximum(b, was), jnp.minimum(b, was)

        def meanwhile():
            @pl.when(r < 3)
            def _():
                far_come(r + 1)

        pairs(12 + r, pick, meanwhile)

    lax.fori_loop(0, 4, far_turn, None)

    far = lax.rem(s + 4, n)
    came(left, side)
    came(right, side)

    @pl.when(core == 0)
    def _():
        pass_on(4, left, side, right).start()

    @pl.when(core == 1)
    def _():
        pass_on(4, right, side, left).start()

    for i, d in enumerate((left, right)):
        pass_across(5 + i, d).start()
        pass_on(7 + i, d, side, sib).start()

    pieces = n * per

    def dest(i):
        return lax.rem(s + 1 + lax.rem(i, n), n), lax.div(i, n)

    def target(frm, part):
        return o_in.at[pl.ds(pl.multiple_of(part * PIECE, PIECE), PIECE), pl.ds(pl.multiple_of(frm * HEAD, HEAD), HEAD)]

    def result(g):
        return q_s.at[lax.div(g, 2), pl.ds(pl.multiple_of(lax.rem(g, 2) * PIECE, PIECE), PIECE)]

    def give(i):
        to, part = dest(i)
        return remote(result(per * to + part), target(s, part), send_o.at[i], recv_o.at[s, part], to)

    def keep(part):
        return pltpu.make_async_copy(result(per * s + part), target(s, part), own_o.at[part])

    def send(i):
        @pl.when(lax.rem(i, n) < n - 1)
        def _():
            give(i).start()

        @pl.when(lax.rem(i, n) == n - 1)
        def _():
            keep(lax.div(i, n)).start()

    def finish(i, _):
        to, part = dest(i)
        g = per * to + part
        mix = mix_s[lax.div(g, 2), :, pl.ds(pl.multiple_of(lax.rem(g, 2) * PIECE, PIECE), PIECE)]
        result(g)[...] = (mix[:HEAD] * (1 / mix[HEAD : HEAD + 1])).T.astype(jnp.bfloat16)

        @pl.when(i > 0)
        def _():
            send(i - 1)

    lax.fori_loop(0, pieces, finish, None)

    for i in range(per):
        swap(i).wait_send()
    for i in range(8):
        remote(own_s.at[0], land.at[0], send_r.at[i], recv_a.at[0], sib).wait_send()
    for i in range(per):
        load_own(i).start()
    send(jnp.int32(pieces - 1))

    came(far, side)
    pass_across(9, far).start()
    pass_on(10, far, side, sib).start()
    for i, d in enumerate((left, right, far)):
        came(d, 1 - side)
        pass_on(11 + i, d, 1 - side, sib).start()
    for h in range(2):
        came(sib, jnp.int32(h))
        for d in (left, right, far):
            came(d + 1 - 2 * core, jnp.int32(h))
    own_out.wait()
    for i in range(per):
        load_own(i).wait()

    for i in range(8):
        forward(8 + i, jnp.int32(0), jnp.int32(0), 0, right).wait_send()
    for i in range(4, 16):
        relay(i, jnp.int32(0)).wait_send()

    def load_out(d):
        return pltpu.make_async_copy(wo_all.at[pl.ds(d * depth, depth)], land.at[d], load_s.at[d])

    for d in range(n):
        load_out(d).start()
    for d in range(n):
        load_out(d).wait()

    width = wo_all.shape[1]
    wide = width // 4

    def out(part):
        return pltpu.make_async_copy(land.at[n + part], y_ref.at[pl.ds(pl.multiple_of(part * PIECE, PIECE), PIECE)], out_s.at[part])

    def last(part, _):
        keep(part).wait()
        for off in range(1, n):
            frm = lax.rem(s + off, n)
            remote(result(jnp.int32(0)), target(frm, part), send_o.at[0], recv_o.at[frm, part], frm).wait_recv()

        def columns(j, _):
            cols = pl.ds(pl.multiple_of(j * wide, wide), wide)
            y = dot(o_in[pl.ds(pl.multiple_of(part * PIECE, PIECE), PIECE), :], land[:n, :, cols].reshape(n * HEAD, wide), 1, 0)
            land[n + part, :, cols] = (own_s[part, :, cols].astype(jnp.float32) + y).astype(jnp.bfloat16)

        lax.fori_loop(0, width // wide, columns, None)
        out(part).start()

    lax.fori_loop(0, per, last, None)

    for off in away:
        for m in range(3):
            weight(off, m, s, partner(off, False)).wait_send()
            hand(off, m, partner(off, True), side).wait_send()
    for m in range(3):
        to_sib(m, s, sib).wait_send()
    for i in range(14):
        pass_on(i, jnp.int32(0), jnp.int32(0), sib).wait_send()

    def sent(i, _):
        @pl.when(lax.rem(i, n) < n - 1)
        def _():
            give(i).wait_send()

    lax.fori_loop(0, pieces, sent, None)
    for i in range(per):
        out(jnp.int32(i)).wait()


def layer(n, x, gain, tables, wq, wk, wv, wo):
    own, width = x.shape
    pieces, blocks = n * own // PIECE, n * own // BLOCK
    anywhere, whole = pl.BlockSpec(memory_space=pl.ANY), pl.BlockSpec(memory_space=pltpu.VMEM)
    dma = pltpu.SemaphoreType.DMA
    bf, f32 = jnp.bfloat16, jnp.float32
    tokens, per = n * own, own // PIECE
    y, _ = pl.pallas_call(
        functools.partial(kernel, n),
        in_specs=[anywhere] + [whole] * 5 + [anywhere] * 4,
        out_specs=[anywhere] * 2,
        out_shape=[jax.ShapeDtypeStruct(x.shape, bf), jax.ShapeDtypeStruct((n * HEAD, width), bf)],
        scratch_shapes=[
            pltpu.VMEM((width, 3 * HEAD), bf),
            pltpu.VMEM((per, PIECE, width), bf),
            pltpu.VMEM((7 * per, PIECE, width), bf),
            pltpu.VMEM((blocks, BLOCK, HEAD), bf),
            pltpu.VMEM((blocks, BLOCK, HEAD), bf),
            pltpu.VMEM((blocks, HEAD, BLOCK), bf),
            pltpu.VMEM((blocks, HEAD + 8, BLOCK), f32),
            pltpu.VMEM((blocks, BLOCK), f32),
            pltpu.VMEM((BLOCK, BLOCK), f32),
            pltpu.VMEM((BLOCK, BLOCK), f32),
            pltpu.VMEM((own, n * HEAD), bf),
            dma((2 * n, 3)), dma((2 * n, 3)), dma((3,)), dma((16,)), dma((7 * per,)), dma((4, 2)), dma((n,)), dma((16,)),
            dma((pieces,)), dma((n, per)), dma((per,)), dma((14,)), dma((n, 2)), dma, dma((per,)),
        ],
        compiler_params=pltpu.CompilerParams(collective_id=0, has_side_effects=True, vmem_limit_bytes=VMEM),
        cost_estimate=pl.CostEstimate(flops=2 * tokens * width * 4 * HEAD + 2 * tokens * tokens * HEAD,
                                      bytes_accessed=2 * tokens * width * 2, transcendentals=tokens * tokens // 2),
    )(x, gain, *tables, wq, wk, wv, wo)
    return y


def tables(tokens):
    speed = float(THETA) ** (-np.arange(HEAD // 2) / (HEAD // 2))
    near, far = np.arange(NEAR)[:, None] * speed, np.arange(0, tokens, NEAR)[:, None] * speed
    return tuple(jnp.asarray(f(t), jnp.float32) for t in (near, far) for f in (np.cos, np.sin))


def solution(mesh):
    n = mesh.shape["sp"]

    def step(x, gain, wq, wk, wv, wo):
        return layer(n, x, gain, tables(n * x.shape[0]), wq, wk, wv, wo)

    tokens, whole = P(("dp", "sp"), None), P("sp", None)
    return jax.shard_map(
        step,
        mesh=mesh,
        in_specs=(tokens, P(None), whole, whole, whole, whole),
        out_specs=tokens,
        check_vma=False,
    )
```

```python
import functools

import jax
import jax.numpy as jnp
import numpy as np
from jax import lax
from jax.experimental import pallas as pl
from jax.experimental.pallas import tpu as pltpu
from jax.sharding import PartitionSpec as P

MESH = pl.DeviceIdType.MESH
HEAD = 256
THETA = 10000
PIECE = 256
BLOCK = 512
STRIP = 256
NEAR = 128
HIDDEN = -2e30
LOG2E = 1.4426950408889634
VMEM = 67043328


def dot(a, b, ca, cb):
    return lax.dot_general(a, b, (((ca,), (cb,)), ((), ())), preferred_element_type=jnp.float32)


def kernel(n, x_ref, gain, cosr, sinr, cosp, sinp, wq, wk, wv, wo, y_ref, wo_all,
           w_s, own_s, land, q_s, k_s, v_s, mix_s, top_s, s0, s1, o_in,
           send_w, recv_w, own_w, send_a, recv_a, recv_f, load_s, send_r, send_o, recv_o, own_o, send_wo, recv_wo, own_wo, out_s):
    s, group = lax.axis_index("sp"), lax.axis_index("dp")
    core, chip = lax.rem(s, 2), lax.div(s, 2)
    chips = n // 2
    sib = s + 1 - 2 * core
    right, left = lax.rem(s + 2, n), lax.rem(s + n - 2, n)
    side = lax.rem(group, 2)
    other = group + 1 - 2 * side
    per = x_ref.shape[0] // PIECE
    depth = wq.shape[0]
    half = depth // 2
    e = HEAD**-0.5 * LOG2E

    def remote(src, dst, ss, rs, to):
        return pltpu.make_async_remote_copy(src_ref=src, dst_ref=dst, send_sem=ss, recv_sem=rs, device_id={"sp": to}, device_id_type=MESH)

    def across(src, dst, ss, rs):
        return pltpu.make_async_remote_copy(src_ref=src, dst_ref=dst, send_sem=ss, recv_sem=rs, device_id={"dp": other}, device_id_type=MESH)

    def load_own(i):
        return pltpu.make_async_copy(x_ref.at[pl.ds(i * PIECE, PIECE)], own_s.at[i], load_s.at[i])

    for i in range(per):
        load_own(i).start()

    barrier = pltpu.get_barrier_semaphore()
    for off in range(1, n):
        pl.semaphore_signal(barrier, inc=1, device_id={"sp": lax.rem(s + off, n)}, device_id_type=MESH)
    pl.semaphore_signal(barrier, inc=1, device_id={"dp": other}, device_id_type=MESH)
    pl.semaphore_wait(barrier, n)

    def rows(d, h):
        return pl.ds(pl.multiple_of(d * depth + h * half, half), half)

    def weight(off, m, frm, to):
        w = (wq, wk, wv)[m]
        return remote(w.at[pl.ds(pl.multiple_of(side * half, half), half), pl.ds(pl.multiple_of(to * HEAD, HEAD), HEAD)],
                      w_s.at[rows(frm, side), pl.ds(m * HEAD, HEAD)], send_w.at[off, m], recv_w.at[off, m], to)

    def hand(off, m, frm, h):
        part = w_s.at[rows(frm, h), pl.ds(m * HEAD, HEAD)]
        return across(part, part, send_w.at[n + off, m], recv_w.at[n + off, m])

    def to_sib(m, frm, to):
        w = (wq, wk, wv)[m]
        return remote(w.at[:, pl.ds(pl.multiple_of(to * HEAD, HEAD), HEAD)],
                      w_s.at[pl.ds(pl.multiple_of(frm * depth, depth), depth), pl.ds(m * HEAD, HEAD)], send_w.at[0, m], recv_w.at[0, m], to)

    away = [2, 6, 4, 3, 7, 5]

    def partner(off, back):
        base = lax.rem(s + (n - (off - off % 2) if back else off - off % 2), n)
        return base + 1 - 2 * core if off % 2 else base

    for off in away:
        for m in range(3):
            weight(off, m, s, partner(off, False)).start()
    for m in range(3):
        to_sib(m, s, sib).start()
    own_weights = [pltpu.make_async_copy(w.at[:, pl.ds(pl.multiple_of(s * HEAD, HEAD), HEAD)],
                                         w_s.at[pl.ds(pl.multiple_of(s * depth, depth), depth), pl.ds(m * HEAD, HEAD)],
                                         own_w.at[m]) for m, w in enumerate((wq, wk, wv))]
    for c in own_weights:
        c.start()
    own_out = pltpu.make_async_copy(wo, wo_all.at[pl.ds(pl.multiple_of(s * depth, depth), depth)], own_wo)
    own_out.start()

    def from_left(b, by):
        return 4 * b + by

    def from_right(b, by):
        return 4 * b + 2 + by

    def from_far(b, by):
        return 16 + 2 * b + by

    def from_sib(i):
        return 24 + i

    def swap(i):
        return remote(own_s.at[i], land.at[from_sib(i)], send_a.at[i], recv_a.at[from_sib(i)], sib)

    def norm(i, rows_at_once=32):
        def some(j, _):
            at = pl.ds(pl.multiple_of(j * rows_at_once, rows_at_once), rows_at_once)
            wide = own_s[i, at, :].astype(jnp.float32)
            scale = lax.rsqrt(jnp.mean(wide * wide, -1, keepdims=True) + 1e-6)
            own_s[i, at, :] = (wide * scale * gain[...].astype(jnp.float32)[None]).astype(jnp.bfloat16)

        lax.fori_loop(0, PIECE // rows_at_once, some, None)

    for i in range(per):
        load_own(i).wait()
        norm(i)
        if i:
            swap(i - 1).start()
    swap(per - 1).start()

    def arrived(slot):
        remote(land.at[slot], land.at[slot], send_a.at[0], recv_a.at[slot], sib).wait_recv()

    for b in range(2):
        arrived(from_sib(2 * b + core))

    def ring(i, b, to, slot):
        mine = core == b // 2

        @pl.when(mine)
        def _():
            remote(own_s.at[2 * (b % 2) + core], land.at[slot], send_r.at[i], recv_a.at[slot], to).start()

        @pl.when(jnp.logical_not(mine))
        def _():
            remote(land.at[from_sib(2 * (b % 2) + core)], land.at[slot], send_r.at[i], recv_a.at[slot], to).start()

    for b in range(4):
        ring(b, b, right, from_left(b, core))
        ring(4 + b, b, left, from_right(b, core))

    for off in away:
        frm = partner(off, True)
        for m in range(3):
            weight(off, m, frm, s).wait_recv()
            hand(off, m, frm, side).start()

    def project(piece, g):
        y = dot(piece, w_s[...], 1, 0)
        cr, sr, turns = cosr[...], sinr[...], []
        for h in range(PIECE // NEAR):
            at = pl.ds(g * (PIECE // NEAR) + h, 1)
            cp, sp = cosp[at, :], sinp[at, :]
            turns.append((cp * cr - sp * sr, sp * cr + cp * sr))
        cos, sin = (jnp.concatenate(t, 0) for t in zip(*turns))
        b, at = lax.div(g, 2), pl.multiple_of(lax.rem(g, 2) * PIECE, PIECE)
        for ref, first in ((q_s, 0), (k_s, HEAD)):
            t = y[:, first : first + HEAD].astype(jnp.bfloat16).astype(jnp.float32)
            lo, hi = t[:, : HEAD // 2], t[:, HEAD // 2 :]
            ref[b, pl.ds(at, PIECE), :] = jnp.concatenate([lo * cos - hi * sin, hi * cos + lo * sin], -1).astype(jnp.bfloat16)
        v_s[b, :, pl.ds(at, PIECE)] = y[:, 2 * HEAD :].astype(jnp.bfloat16).T

    def diagonal(g):
        for h in range(BLOCK // STRIP):
            seen, cols = (h + 1) * STRIP, slice(h * STRIP, (h + 1) * STRIP)
            t = dot(k_s[g, :seen, :], q_s[g, cols, :], 1, 1)
            ok = lax.broadcasted_iota(jnp.int32, t.shape, 1) + h * STRIP >= lax.broadcasted_iota(jnp.int32, t.shape, 0)
            t = jnp.where(ok, t, HIDDEN)
            top = t.max(axis=0, keepdims=True)
            top_s[pl.ds(g, 1), cols] = top
            values = jnp.concatenate([v_s[g, :, :seen], jnp.ones((8, seen), jnp.bfloat16)], 0)
            mix_s[g, :, cols] = dot(values, jnp.exp2((t - top) * e).astype(jnp.bfloat16), 1, 0)

    def scores(pair):
        return dot(k_s[pair[1]], q_s[pair[0]], 1, 1)

    def pair_step(now, later, pair, following):
        later[...] = scores(following)
        q, k = pair
        values = jnp.concatenate([v_s[k], jnp.ones((8, BLOCK), jnp.bfloat16)], 0)
        for h in range(BLOCK // STRIP):
            cols = slice(h * STRIP, (h + 1) * STRIP)
            t = now[:, cols]
            old = top_s[pl.ds(q, 1), cols]
            top = jnp.maximum(old, t.max(axis=0, keepdims=True))
            top_s[pl.ds(q, 1), cols] = top
            p = jnp.exp2((t - top) * e).astype(jnp.bfloat16)
            mix_s[q, :, cols] = mix_s[q, :, cols] * jnp.exp2((old - top) * e) + dot(values, p, 1, 0)

    def pairs(count, pick, meanwhile):
        s0[...] = scores(pick(jnp.int32(0)))
        turns = lax.div(count + 1, 2)

        def body(u, _):
            t = 2 * u

            @pl.when(u == jnp.maximum(turns - 3, 0))
            def _():
                meanwhile()

            pair_step(s0, s1, pick(t), pick(jnp.minimum(t + 1, count - 1)))

            @pl.when(t + 1 < count)
            def _():
                pair_step(s1, s0, pick(t + 1), pick(jnp.minimum(t + 2, count - 1)))

        lax.fori_loop(0, turns, body, None)

    first = 4 * chip
    chip_left, chip_right, chip_far = (4 * lax.rem(chip + d, chips) for d in (chips - 1, 1, 2))

    def old(i):
        near = jnp.where(lax.rem(i, 2) == 0, chip_left, chip_right) + lax.div(i - 4, 2)
        return jnp.where(i < 4, first + i, jnp.where(i < 12, near, chip_far + i - 12))

    def relay(i, slot):
        return remote(land.at[slot], land.at[slot], send_a.at[i], recv_a.at[slot], sib)

    def forward(i, slot, b, h, to):
        at = pl.ds(h * (PIECE // 2), PIECE // 2)
        return remote(land.at[slot, at], land.at[from_far(b, core), at], send_r.at[i], recv_f.at[b, h], to)

    def near_come(b):
        for i, slot in enumerate((from_left(b, core), from_right(b, core))):
            arrived(slot)
            relay(4 + 2 * b + i, slot).start()
            forward(8 + 2 * b + i, slot, b, i, (right, left)[i]).start()

    def far_come(b):
        for h in range(2):
            forward(0, jnp.int32(0), b, h, sib).wait_recv()
        relay(12 + b, from_far(b, core)).start()

    for c in own_weights:
        c.wait()
    for m in range(3):
        to_sib(m, sib, s).wait_recv()
    for off in away:
        for m in range(3):
            hand(off, m, partner(off, True), 1 - side).wait_recv()
    lax.fori_loop(0, per, lambda i, _: project(own_s[i], per * s + i), None)
    for b in range(2):
        arrived(from_sib(2 * b + 1 - core))
    lax.fori_loop(0, per, lambda i, _: project(land[from_sib(i)], per * sib + i), None)
    lax.fori_loop(0, 4, lambda b, _: diagonal(first + b), None)

    def pick_own(t):
        q = 1 + (t >= 1).astype(jnp.int32) + (t >= 3).astype(jnp.int32)
        return first + q, first + t - lax.div(q * (q - 1), 2)

    pairs(jnp.int32(6), pick_own, lambda: near_come(jnp.int32(0)))

    def turn(r, _):
        blocks = chip_left + r, chip_right + r

        def go(i, _):
            by = jnp.where(i < 2, core, 1 - core)

            @pl.when(i == 2)
            def _():
                arrived(from_left(r, 1 - core))
                arrived(from_right(r, 1 - core))

            even = lax.rem(i, 2) == 0
            project(land[jnp.where(even, from_left(r, by), from_right(r, by))], 2 * jnp.where(even, blocks[0], blocks[1]) + by)

        lax.fori_loop(0, 4, go, None)
        lax.fori_loop(0, 2, lambda i, _: diagonal(jnp.where(i == 0, blocks[0], blocks[1])), None)

        def pick(t):
            new = jnp.where(lax.rem(t, 2) == 0, blocks[1], blocks[0])
            was = old(lax.div(t, 2))
            return jnp.maximum(new, was), jnp.minimum(new, was)

        def meanwhile():
            @pl.when(r < 3)
            def _():
                near_come(r + 1)

            @pl.when(r == 3)
            def _():
                far_come(jnp.int32(0))

        pairs(9 + 4 * r, pick, meanwhile)

    lax.fori_loop(0, 4, turn, None)

    def out_rows(d, h):
        return wo_all.at[rows(d, h)]

    def out_own(i, h, to):
        return remote(wo.at[pl.ds(pl.multiple_of(h * half, half), half)], out_rows(s, h), send_wo.at[i], recv_wo.at[s, h], to)

    def came(d, h):
        remote(out_rows(d, h), out_rows(d, h), send_wo.at[0], recv_wo.at[d, h], sib).wait_recv()

    def pass_on(i, d, h, to):
        return remote(out_rows(d, h), out_rows(d, h), send_wo.at[i], recv_wo.at[d, h], to)

    def pass_across(i, d):
        return across(out_rows(d, side), out_rows(d, side), send_wo.at[i], recv_wo.at[d, side])

    out_own(0, side, right).start()
    out_own(1, side, left).start()
    out_own(2, jnp.int32(0), sib).start()
    out_own(3, jnp.int32(1), sib).start()

    far = lax.rem(s + 4, n)

    def out_near():
        came(left, side)
        came(right, side)

        @pl.when(core == 0)
        def _():
            pass_on(4, left, side, right).start()

        @pl.when(core == 1)
        def _():
            pass_on(4, right, side, left).start()

        for i, d in enumerate((left, right)):
            pass_across(5 + i, d).start()
            pass_on(7 + i, d, side, sib).start()

    def far_turn(r, _):
        b = chip_far + r

        def go(i, _):
            by = jnp.where(i == 0, core, 1 - core)

            @pl.when(i == 1)
            def _():
                arrived(from_far(r, 1 - core))

            project(land[from_far(r, by)], 2 * b + by)

        lax.fori_loop(0, 2, go, None)
        diagonal(b)

        def pick(t):
            was = old(t)
            return jnp.maximum(b, was), jnp.minimum(b, was)

        def meanwhile():
            @pl.when(r < 3)
            def _():
                far_come(r + 1)

            @pl.when(r == 3)
            def _():
                out_near()

        pairs(12 + r, pick, meanwhile)

    lax.fori_loop(0, 4, far_turn, None)

    pieces = n * per

    def dest(i):
        return lax.rem(s + 1 + lax.rem(i, n), n), lax.div(i, n)

    def target(frm, part):
        return o_in.at[pl.ds(pl.multiple_of(part * PIECE, PIECE), PIECE), pl.ds(pl.multiple_of(frm * HEAD, HEAD), HEAD)]

    def result(g):
        return q_s.at[lax.div(g, 2), pl.ds(pl.multiple_of(lax.rem(g, 2) * PIECE, PIECE), PIECE)]

    def give(i):
        to, part = dest(i)
        return remote(result(per * to + part), target(s, part), send_o.at[i], recv_o.at[s, part], to)

    def keep(part):
        return pltpu.make_async_copy(result(per * s + part), target(s, part), own_o.at[part])

    def send(i):
        @pl.when(lax.rem(i, n) < n - 1)
        def _():
            give(i).start()

        @pl.when(lax.rem(i, n) == n - 1)
        def _():
            keep(lax.div(i, n)).start()

    def finish(i, _):
        to, part = dest(i)
        g = per * to + part
        mix = mix_s[lax.div(g, 2), :, pl.ds(pl.multiple_of(lax.rem(g, 2) * PIECE, PIECE), PIECE)]
        result(g)[...] = (mix[:HEAD] * (1 / mix[HEAD : HEAD + 1])).T.astype(jnp.bfloat16)

        @pl.when(i > 0)
        def _():
            send(i - 1)

    lax.fori_loop(0, pieces, finish, None)

    for i in range(per):
        swap(i).wait_send()
    for i in range(8):
        remote(own_s.at[0], land.at[0], send_r.at[i], recv_a.at[0], sib).wait_send()
    for i in range(per):
        load_own(i).start()
    send(jnp.int32(pieces - 1))

    came(far, side)
    pass_across(9, far).start()
    pass_on(10, far, side, sib).start()
    for i, d in enumerate((left, right, far)):
        came(d, 1 - side)
        pass_on(11 + i, d, 1 - side, sib).start()
    for h in range(2):
        came(sib, jnp.int32(h))
        for d in (left, right, far):
            came(d + 1 - 2 * core, jnp.int32(h))
    own_out.wait()
    for i in range(per):
        load_own(i).wait()

    for i in range(8):
        forward(8 + i, jnp.int32(0), jnp.int32(0), 0, right).wait_send()
    for i in range(4, 16):
        relay(i, jnp.int32(0)).wait_send()

    def load_out(d):
        return pltpu.make_async_copy(wo_all.at[pl.ds(d * depth, depth)], land.at[d], load_s.at[d])

    for d in range(n):
        load_out(d).start()
    for d in range(n):
        load_out(d).wait()

    width = wo_all.shape[1]
    wide = width // 4

    def out(part, j):
        cols = pl.ds(pl.multiple_of(j * wide, wide), wide)
        return pltpu.make_async_copy(land.at[n + part, :, cols], y_ref.at[pl.ds(pl.multiple_of(part * PIECE, PIECE), PIECE), cols],
                                     out_s.at[part, j])

    def last(part, _):
        keep(part).wait()
        for off in range(1, n):
            frm = lax.rem(s + off, n)
            remote(result(jnp.int32(0)), target(frm, part), send_o.at[0], recv_o.at[frm, part], frm).wait_recv()

        def columns(j, _):
            cols = pl.ds(pl.multiple_of(j * wide, wide), wide)
            y = dot(o_in[pl.ds(pl.multiple_of(part * PIECE, PIECE), PIECE), :], land[:n, :, cols].reshape(n * HEAD, wide), 1, 0)
            land[n + part, :, cols] = (own_s[part, :, cols].astype(jnp.float32) + y).astype(jnp.bfloat16)
            out(part, j).start()

        lax.fori_loop(0, width // wide, columns, None)

    lax.fori_loop(0, per, last, None)

    for off in away:
        for m in range(3):
            weight(off, m, s, partner(off, False)).wait_send()
            hand(off, m, partner(off, True), side).wait_send()
    for m in range(3):
        to_sib(m, s, sib).wait_send()
    for i in range(14):
        pass_on(i, jnp.int32(0), jnp.int32(0), sib).wait_send()

    def sent(i, _):
        @pl.when(lax.rem(i, n) < n - 1)
        def _():
            give(i).wait_send()

    lax.fori_loop(0, pieces, sent, None)
    for i in range(per):
        for j in range(width // wide):
            out(jnp.int32(i), jnp.int32(j)).wait()


def layer(n, x, gain, tables, wq, wk, wv, wo):
    own, width = x.shape
    pieces, blocks = n * own // PIECE, n * own // BLOCK
    anywhere, whole = pl.BlockSpec(memory_space=pl.ANY), pl.BlockSpec(memory_space=pltpu.VMEM)
    dma = pltpu.SemaphoreType.DMA
    bf, f32 = jnp.bfloat16, jnp.float32
    tokens, per = n * own, own // PIECE
    y, _ = pl.pallas_call(
        functools.partial(kernel, n),
        in_specs=[anywhere] + [whole] * 5 + [anywhere] * 4,
        out_specs=[anywhere] * 2,
        out_shape=[jax.ShapeDtypeStruct(x.shape, bf), jax.ShapeDtypeStruct((n * HEAD, width), bf)],
        scratch_shapes=[
            pltpu.VMEM((width, 3 * HEAD), bf),
            pltpu.VMEM((per, PIECE, width), bf),
            pltpu.VMEM((7 * per, PIECE, width), bf),
            pltpu.VMEM((blocks, BLOCK, HEAD), bf),
            pltpu.VMEM((blocks, BLOCK, HEAD), bf),
            pltpu.VMEM((blocks, HEAD, BLOCK), bf),
            pltpu.VMEM((blocks, HEAD + 8, BLOCK), f32),
            pltpu.VMEM((blocks, BLOCK), f32),
            pltpu.VMEM((BLOCK, BLOCK), f32),
            pltpu.VMEM((BLOCK, BLOCK), f32),
            pltpu.VMEM((own, n * HEAD), bf),
            dma((2 * n, 3)), dma((2 * n, 3)), dma((3,)), dma((16,)), dma((7 * per,)), dma((4, 2)), dma((n,)), dma((16,)),
            dma((pieces,)), dma((n, per)), dma((per,)), dma((14,)), dma((n, 2)), dma, dma((per, 4)),
        ],
        compiler_params=pltpu.CompilerParams(collective_id=0, has_side_effects=True, vmem_limit_bytes=VMEM),
        cost_estimate=pl.CostEstimate(flops=2 * tokens * width * 4 * HEAD + 2 * tokens * tokens * HEAD,
                                      bytes_accessed=2 * tokens * width * 2, transcendentals=tokens * tokens // 2),
    )(x, gain, *tables, wq, wk, wv, wo)
    return moved(y)


def moved(y):
    parts = 8
    rows = y.shape[0] // parts

    def body(y_ref, out_ref, buffer, took, gave):
        def take(i):
            return pltpu.make_async_copy(y_ref.at[pl.ds(i * rows, rows)], buffer.at[i], took.at[i])

        def give(i):
            return pltpu.make_async_copy(buffer.at[i], out_ref.at[pl.ds(i * rows, rows)], gave.at[i])

        for i in range(parts):
            take(i).start()
        for i in range(parts):
            take(i).wait()
            give(i).start()
        for i in range(parts):
            give(i).wait()

    return pl.pallas_call(
        body,
        in_specs=[pl.BlockSpec(memory_space=pl.ANY)],
        out_specs=pl.BlockSpec(memory_space=pl.ANY),
        out_shape=jax.ShapeDtypeStruct(y.shape, y.dtype),
        scratch_shapes=[pltpu.VMEM((parts, rows, y.shape[1]), y.dtype), pltpu.SemaphoreType.DMA((parts,)), pltpu.SemaphoreType.DMA((parts,))],
        compiler_params=pltpu.CompilerParams(vmem_limit_bytes=VMEM),
    )(y)


def tables(tokens):
    speed = float(THETA) ** (-np.arange(HEAD // 2) / (HEAD // 2))
    near, far = np.arange(NEAR)[:, None] * speed, np.arange(0, tokens, NEAR)[:, None] * speed
    return tuple(jnp.asarray(f(t), jnp.float32) for t in (near, far) for f in (np.cos, np.sin))


def solution(mesh):
    n = mesh.shape["sp"]

    def step(x, gain, wq, wk, wv, wo):
        return layer(n, x, gain, tables(n * x.shape[0]), wq, wk, wv, wo)

    tokens, whole = P(("dp", "sp"), None), P("sp", None)
    return jax.shard_map(
        step,
        mesh=mesh,
        in_specs=(tokens, P(None), whole, whole, whole, whole),
        out_specs=tokens,
        check_vma=False,
    )
```

```python
import functools

import jax
import jax.numpy as jnp
import numpy as np
from jax import lax
from jax.experimental import pallas as pl
from jax.experimental.pallas import tpu as pltpu
from jax.sharding import PartitionSpec as P

MESH = pl.DeviceIdType.MESH
HEAD = 256
THETA = 10000
PIECE = 256
BLOCK = 512
STRIP = 256
NEAR = 128
HIDDEN = -2e30
LOG2E = 1.4426950408889634
VMEM = 67043328


def dot(a, b, ca, cb):
    return lax.dot_general(a, b, (((ca,), (cb,)), ((), ())), preferred_element_type=jnp.float32)


def kernel(n, x_ref, gain, cosr, sinr, cosp, sinp, wq, wk, wv, wo, y_ref, wo_all,
           w_s, own_s, land, q_s, k_s, v_s, mix_s, top_s, s0, s1, o_in,
           send_w, recv_w, own_w, send_a, recv_a, recv_f, load_s, send_r, send_o, recv_o, own_o, send_wo, recv_wo, own_wo, out_s):
    s, group = lax.axis_index("sp"), lax.axis_index("dp")
    core, chip = lax.rem(s, 2), lax.div(s, 2)
    chips = n // 2
    sib = s + 1 - 2 * core
    right, left = lax.rem(s + 2, n), lax.rem(s + n - 2, n)
    side = lax.rem(group, 2)
    other = group + 1 - 2 * side
    per = x_ref.shape[0] // PIECE
    depth = wq.shape[0]
    half = depth // 2
    e = HEAD**-0.5 * LOG2E

    def remote(src, dst, ss, rs, to):
        return pltpu.make_async_remote_copy(src_ref=src, dst_ref=dst, send_sem=ss, recv_sem=rs, device_id={"sp": to}, device_id_type=MESH)

    def across(src, dst, ss, rs):
        return pltpu.make_async_remote_copy(src_ref=src, dst_ref=dst, send_sem=ss, recv_sem=rs, device_id={"dp": other}, device_id_type=MESH)

    def load_own(i):
        return pltpu.make_async_copy(x_ref.at[pl.ds(i * PIECE, PIECE)], own_s.at[i], load_s.at[i])

    for i in range(per):
        load_own(i).start()

    barrier = pltpu.get_barrier_semaphore()
    for off in range(1, n):
        pl.semaphore_signal(barrier, inc=1, device_id={"sp": lax.rem(s + off, n)}, device_id_type=MESH)
    pl.semaphore_signal(barrier, inc=1, device_id={"dp": other}, device_id_type=MESH)
    pl.semaphore_wait(barrier, n)

    def rows(d, h):
        return pl.ds(pl.multiple_of(d * depth + h * half, half), half)

    def weight(off, m, frm, to):
        w = (wq, wk, wv)[m]
        return remote(w.at[pl.ds(pl.multiple_of(side * half, half), half), pl.ds(pl.multiple_of(to * HEAD, HEAD), HEAD)],
                      w_s.at[rows(frm, side), pl.ds(m * HEAD, HEAD)], send_w.at[off, m], recv_w.at[off, m], to)

    def hand(off, m, frm, h):
        part = w_s.at[rows(frm, h), pl.ds(m * HEAD, HEAD)]
        return across(part, part, send_w.at[n + off, m], recv_w.at[n + off, m])

    def to_sib(m, frm, to):
        w = (wq, wk, wv)[m]
        return remote(w.at[:, pl.ds(pl.multiple_of(to * HEAD, HEAD), HEAD)],
                      w_s.at[pl.ds(pl.multiple_of(frm * depth, depth), depth), pl.ds(m * HEAD, HEAD)], send_w.at[0, m], recv_w.at[0, m], to)

    away = [2, 6, 4, 3, 7, 5]

    def partner(off, back):
        base = lax.rem(s + (n - (off - off % 2) if back else off - off % 2), n)
        return base + 1 - 2 * core if off % 2 else base

    for off in away:
        for m in range(3):
            weight(off, m, s, partner(off, False)).start()
    for m in range(3):
        to_sib(m, s, sib).start()
    own_weights = [pltpu.make_async_copy(w.at[:, pl.ds(pl.multiple_of(s * HEAD, HEAD), HEAD)],
                                         w_s.at[pl.ds(pl.multiple_of(s * depth, depth), depth), pl.ds(m * HEAD, HEAD)],
                                         own_w.at[m]) for m, w in enumerate((wq, wk, wv))]
    for c in own_weights:
        c.start()
    own_out = pltpu.make_async_copy(wo, wo_all.at[pl.ds(pl.multiple_of(s * depth, depth), depth)], own_wo)
    own_out.start()

    def from_left(b, by):
        return 4 * b + by

    def from_right(b, by):
        return 4 * b + 2 + by

    def from_far(b, by):
        return 16 + 2 * b + by

    def from_sib(i):
        return 24 + i

    def swap(i):
        return remote(own_s.at[i], land.at[from_sib(i)], send_a.at[i], recv_a.at[from_sib(i)], sib)

    def norm(i, rows_at_once=32):
        def some(j, _):
            at = pl.ds(pl.multiple_of(j * rows_at_once, rows_at_once), rows_at_once)
            wide = own_s[i, at, :].astype(jnp.float32)
            scale = lax.rsqrt(jnp.mean(wide * wide, -1, keepdims=True) + 1e-6)
            own_s[i, at, :] = (wide * scale * gain[...].astype(jnp.float32)[None]).astype(jnp.bfloat16)

        lax.fori_loop(0, PIECE // rows_at_once, some, None)

    for i in range(per):
        load_own(i).wait()
        norm(i)
        if i:
            swap(i - 1).start()
    swap(per - 1).start()

    def arrived(slot):
        remote(land.at[slot], land.at[slot], send_a.at[0], recv_a.at[slot], sib).wait_recv()

    for b in range(2):
        arrived(from_sib(2 * b + core))

    def ring(i, b, to, slot):
        mine = core == b // 2

        @pl.when(mine)
        def _():
            remote(own_s.at[2 * (b % 2) + core], land.at[slot], send_r.at[i], recv_a.at[slot], to).start()

        @pl.when(jnp.logical_not(mine))
        def _():
            remote(land.at[from_sib(2 * (b % 2) + core)], land.at[slot], send_r.at[i], recv_a.at[slot], to).start()

    for b in range(4):
        ring(b, b, right, from_left(b, core))
        ring(4 + b, b, left, from_right(b, core))

    for off in away:
        frm = partner(off, True)
        for m in range(3):
            weight(off, m, frm, s).wait_recv()
            hand(off, m, frm, side).start()

    def project(piece, g):
        y = dot(piece, w_s[...], 1, 0)
        cr, sr, turns = cosr[...], sinr[...], []
        for h in range(PIECE // NEAR):
            at = pl.ds(g * (PIECE // NEAR) + h, 1)
            cp, sp = cosp[at, :], sinp[at, :]
            turns.append((cp * cr - sp * sr, sp * cr + cp * sr))
        cos, sin = (jnp.concatenate(t, 0) for t in zip(*turns))
        b, at = lax.div(g, 2), pl.multiple_of(lax.rem(g, 2) * PIECE, PIECE)
        for ref, first in ((q_s, 0), (k_s, HEAD)):
            t = y[:, first : first + HEAD].astype(jnp.bfloat16).astype(jnp.float32)
            lo, hi = t[:, : HEAD // 2], t[:, HEAD // 2 :]
            ref[b, pl.ds(at, PIECE), :] = jnp.concatenate([lo * cos - hi * sin, hi * cos + lo * sin], -1).astype(jnp.bfloat16)
        v_s[b, :, pl.ds(at, PIECE)] = y[:, 2 * HEAD :].astype(jnp.bfloat16).T

    def diagonal(g):
        strips = [((h + 1) * STRIP, slice(h * STRIP, (h + 1) * STRIP)) for h in range(BLOCK // STRIP)]
        found = [dot(k_s[g, :seen, :], q_s[g, cols, :], 1, 1) for seen, cols in strips]
        tops, weights = [], []
        for (seen, cols), t in zip(strips, found):
            ok = lax.broadcasted_iota(jnp.int32, t.shape, 1) + cols.start >= lax.broadcasted_iota(jnp.int32, t.shape, 0)
            t = jnp.where(ok, t, HIDDEN)
            tops.append(t.max(axis=0, keepdims=True))
            weights.append(jnp.exp2((t - tops[-1]) * e).astype(jnp.bfloat16))
        for (seen, cols), top, p in zip(strips, tops, weights):
            top_s[g, :, cols] = top
            mix_s[g, :, cols] = dot(jnp.concatenate([v_s[g, :, :seen], jnp.ones((8, seen), jnp.bfloat16)], 0), p, 1, 0)

    def scores(pair):
        return dot(k_s[pair[1]], q_s[pair[0]], 1, 1)

    def pair_step(now, later, pair, following):
        q, k = pair
        values = jnp.concatenate([v_s[k], jnp.ones((8, BLOCK), jnp.bfloat16)], 0)
        new = scores(following)
        later[...] = new
        olds = top_s[q]
        tops = jnp.maximum(olds, now[...].max(axis=0, keepdims=True))
        top_s[q] = tops
        keeps = jnp.exp2((olds - tops) * e)
        for h in range(BLOCK // STRIP):
            cols = slice(h * STRIP, (h + 1) * STRIP)
            p = jnp.exp2((now[:, cols] - tops[:, cols]) * e).astype(jnp.bfloat16)
            mix_s[q, :, cols] = mix_s[q, :, cols] * keeps[:, cols] + dot(values, p, 1, 0)

    def pairs(count, pick, meanwhile, before=lambda: None):
        s0[...] = scores(pick(jnp.int32(0)))
        before()
        turns = lax.div(count + 1, 2)

        def body(u, _):
            t = 2 * u

            @pl.when(u == jnp.maximum(turns - 5, 0))
            def _():
                meanwhile()

            pair_step(s0, s1, pick(t), pick(jnp.minimum(t + 1, count - 1)))

            @pl.when(t + 1 < count)
            def _():
                pair_step(s1, s0, pick(t + 1), pick(jnp.minimum(t + 2, count - 1)))

        lax.fori_loop(0, turns, body, None)

    first = 4 * chip
    chip_left, chip_right, chip_far = (4 * lax.rem(chip + d, chips) for d in (chips - 1, 1, 2))

    def old(i):
        near = jnp.where(lax.rem(i, 2) == 0, chip_left, chip_right) + lax.div(i - 4, 2)
        return jnp.where(i < 4, first + i, jnp.where(i < 12, near, chip_far + i - 12))

    def relay(i, slot):
        return remote(land.at[slot], land.at[slot], send_a.at[i], recv_a.at[slot], sib)

    def forward(i, slot, b, h, to):
        at = pl.ds(h * (PIECE // 2), PIECE // 2)
        return remote(land.at[slot, at], land.at[from_far(b, core), at], send_r.at[i], recv_f.at[b, h], to)

    def near_come(b):
        for i, slot in enumerate((from_left(b, core), from_right(b, core))):
            arrived(slot)
            relay(4 + 2 * b + i, slot).start()
            forward(8 + 2 * b + i, slot, b, i, (right, left)[i]).start()

    def far_come(b):
        for h in range(2):
            forward(0, jnp.int32(0), b, h, sib).wait_recv()
        relay(12 + b, from_far(b, core)).start()

    for c in own_weights:
        c.wait()
    for m in range(3):
        to_sib(m, sib, s).wait_recv()
    for off in away:
        for m in range(3):
            hand(off, m, partner(off, True), 1 - side).wait_recv()
    lax.fori_loop(0, per, lambda i, _: project(own_s[i], per * s + i), None)
    for b in range(2):
        arrived(from_sib(2 * b + 1 - core))
    lax.fori_loop(0, per, lambda i, _: project(land[from_sib(i)], per * sib + i), None)
    lax.fori_loop(0, 4, lambda b, _: diagonal(first + b), None)

    def pick_own(t):
        q = 1 + (t >= 1).astype(jnp.int32) + (t >= 3).astype(jnp.int32)
        return first + q, first + t - lax.div(q * (q - 1), 2)

    pairs(jnp.int32(6), pick_own, lambda: near_come(jnp.int32(0)))

    def turn(r, _):
        blocks = chip_left + r, chip_right + r

        def go(i, _):
            by = jnp.where(i < 2, core, 1 - core)

            @pl.when(i == 2)
            def _():
                arrived(from_left(r, 1 - core))
                arrived(from_right(r, 1 - core))

            even = lax.rem(i, 2) == 0
            project(land[jnp.where(even, from_left(r, by), from_right(r, by))], 2 * jnp.where(even, blocks[0], blocks[1]) + by)

        lax.fori_loop(0, 4, go, None)
        lax.fori_loop(0, 2, lambda i, _: diagonal(jnp.where(i == 0, blocks[0], blocks[1])), None)

        def pick(t):
            new = jnp.where(lax.rem(t, 2) == 0, blocks[1], blocks[0])
            was = old(lax.div(t, 2))
            return jnp.maximum(new, was), jnp.minimum(new, was)

        def meanwhile():
            @pl.when(r < 3)
            def _():
                near_come(r + 1)

            @pl.when(r == 3)
            def _():
                far_come(jnp.int32(0))

        pairs(9 + 4 * r, pick, meanwhile)

    lax.fori_loop(0, 4, turn, None)

    def out_rows(d, h):
        return wo_all.at[rows(d, h)]

    def out_own(i, h, to):
        return remote(wo.at[pl.ds(pl.multiple_of(h * half, half), half)], out_rows(s, h), send_wo.at[i], recv_wo.at[s, h], to)

    def came(d, h):
        remote(out_rows(d, h), out_rows(d, h), send_wo.at[0], recv_wo.at[d, h], sib).wait_recv()

    def pass_on(i, d, h, to):
        return remote(out_rows(d, h), out_rows(d, h), send_wo.at[i], recv_wo.at[d, h], to)

    def pass_across(i, d):
        return across(out_rows(d, side), out_rows(d, side), send_wo.at[i], recv_wo.at[d, side])

    out_own(0, side, right).start()
    out_own(1, side, left).start()
    out_own(2, jnp.int32(0), sib).start()
    out_own(3, jnp.int32(1), sib).start()

    far = lax.rem(s + 4, n)

    def out_near():
        came(left, side)
        came(right, side)

        @pl.when(core == 0)
        def _():
            pass_on(4, left, side, right).start()

        @pl.when(core == 1)
        def _():
            pass_on(4, right, side, left).start()

        for i, d in enumerate((left, right)):
            pass_across(5 + i, d).start()
            pass_on(7 + i, d, side, sib).start()

    def far_turn(r, _):
        b = chip_far + r

        def go(i, _):
            by = jnp.where(i == 0, core, 1 - core)

            @pl.when(i == 1)
            def _():
                arrived(from_far(r, 1 - core))

            project(land[from_far(r, by)], 2 * b + by)

        lax.fori_loop(0, 2, go, None)

        def pick(t):
            was = old(t)
            return jnp.maximum(b, was), jnp.minimum(b, was)

        def meanwhile():
            @pl.when(r < 3)
            def _():
                far_come(r + 1)

            @pl.when(r == 3)
            def _():
                out_near()

        pairs(12 + r, pick, meanwhile, lambda: diagonal(b))

    lax.fori_loop(0, 4, far_turn, None)

    pieces = n * per

    def dest(i):
        p = lax.rem(i, n)
        p = jnp.where(p < n - 2, lax.rem(p + (n // 2) * (1 - core), n - 2), p)
        on = jnp.where(p < 4, 1 + 2 * lax.rem(p, 2), jnp.where(p < 6, 2, 0))
        flip = jnp.where(p < 4, lax.div(p, 2), jnp.where(p < 6, p - 4, 7 - p))
        to = lax.rem(s + 2 * on, n)
        return to + flip * (1 - 2 * core), lax.div(i, n)

    def target(frm, part):
        return o_in.at[pl.ds(pl.multiple_of(part * PIECE, PIECE), PIECE), pl.ds(pl.multiple_of(frm * HEAD, HEAD), HEAD)]

    def result(g):
        return q_s.at[lax.div(g, 2), pl.ds(pl.multiple_of(lax.rem(g, 2) * PIECE, PIECE), PIECE)]

    def give(i):
        to, part = dest(i)
        return remote(result(per * to + part), target(s, part), send_o.at[i], recv_o.at[s, part], to)

    def keep(part):
        return pltpu.make_async_copy(result(per * s + part), target(s, part), own_o.at[part])

    def send(i):
        @pl.when(lax.rem(i, n) < n - 1)
        def _():
            give(i).start()

        @pl.when(lax.rem(i, n) == n - 1)
        def _():
            keep(lax.div(i, n)).start()

    def finish(i, _):
        to, part = dest(i)
        g = per * to + part
        mix = mix_s[lax.div(g, 2), :, pl.ds(pl.multiple_of(lax.rem(g, 2) * PIECE, PIECE), PIECE)]
        result(g)[...] = (mix[:HEAD] * (1 / mix[HEAD : HEAD + 1])).T.astype(jnp.bfloat16)

        @pl.when(i > 0)
        def _():
            send(i - 1)

    lax.fori_loop(0, pieces, finish, None)

    for i in range(per):
        swap(i).wait_send()
    for i in range(8):
        remote(own_s.at[0], land.at[0], send_r.at[i], recv_a.at[0], sib).wait_send()
    for i in range(per):
        load_own(i).start()
    send(jnp.int32(pieces - 1))

    came(far, side)
    pass_across(9, far).start()
    pass_on(10, far, side, sib).start()
    for i, d in enumerate((left, right, far)):
        came(d, 1 - side)
        pass_on(11 + i, d, 1 - side, sib).start()
    for h in range(2):
        came(sib, jnp.int32(h))
        for d in (left, right, far):
            came(d + 1 - 2 * core, jnp.int32(h))
    own_out.wait()
    for i in range(per):
        load_own(i).wait()

    for i in range(8):
        forward(8 + i, jnp.int32(0), jnp.int32(0), 0, right).wait_send()
    for i in range(4, 16):
        relay(i, jnp.int32(0)).wait_send()

    def load_out(d):
        return pltpu.make_async_copy(wo_all.at[pl.ds(d * depth, depth)], land.at[d], load_s.at[d])

    for d in range(n):
        load_out(d).start()
    for d in range(n):
        load_out(d).wait()

    width = wo_all.shape[1]
    wide = width // 4

    def out(part, j):
        cols = pl.ds(pl.multiple_of(j * wide, wide), wide)
        return pltpu.make_async_copy(land.at[n + part, :, cols], y_ref.at[pl.ds(pl.multiple_of(part * PIECE, PIECE), PIECE), cols],
                                     out_s.at[part, j])

    def last(part, _):
        keep(part).wait()
        for off in range(1, n):
            frm = lax.rem(s + off, n)
            remote(result(jnp.int32(0)), target(frm, part), send_o.at[0], recv_o.at[frm, part], frm).wait_recv()

        def columns(j, _):
            cols = pl.ds(pl.multiple_of(j * wide, wide), wide)
            y = dot(o_in[pl.ds(pl.multiple_of(part * PIECE, PIECE), PIECE), :], land[:n, :, cols].reshape(n * HEAD, wide), 1, 0)
            land[n + part, :, cols] = (own_s[part, :, cols].astype(jnp.float32) + y).astype(jnp.bfloat16)
            out(part, j).start()

        lax.fori_loop(0, width // wide, columns, None)

    lax.fori_loop(0, per, last, None)

    for off in away:
        for m in range(3):
            weight(off, m, s, partner(off, False)).wait_send()
            hand(off, m, partner(off, True), side).wait_send()
    for m in range(3):
        to_sib(m, s, sib).wait_send()
    for i in range(14):
        pass_on(i, jnp.int32(0), jnp.int32(0), sib).wait_send()

    def sent(i, _):
        @pl.when(lax.rem(i, n) < n - 1)
        def _():
            give(i).wait_send()

    lax.fori_loop(0, pieces, sent, None)
    for i in range(per):
        for j in range(width // wide):
            out(jnp.int32(i), jnp.int32(j)).wait()


def layer(n, x, gain, tables, wq, wk, wv, wo):
    own, width = x.shape
    pieces, blocks = n * own // PIECE, n * own // BLOCK
    anywhere, whole = pl.BlockSpec(memory_space=pl.ANY), pl.BlockSpec(memory_space=pltpu.VMEM)
    dma = pltpu.SemaphoreType.DMA
    bf, f32 = jnp.bfloat16, jnp.float32
    tokens, per = n * own, own // PIECE
    y, _ = pl.pallas_call(
        functools.partial(kernel, n),
        in_specs=[anywhere] + [whole] * 5 + [anywhere] * 4,
        out_specs=[anywhere] * 2,
        out_shape=[jax.ShapeDtypeStruct(x.shape, bf), jax.ShapeDtypeStruct((n * HEAD, width), bf)],
        scratch_shapes=[
            pltpu.VMEM((width, 3 * HEAD), bf),
            pltpu.VMEM((per, PIECE, width), bf),
            pltpu.VMEM((7 * per, PIECE, width), bf),
            pltpu.VMEM((blocks, BLOCK, HEAD), bf),
            pltpu.VMEM((blocks, BLOCK, HEAD), bf),
            pltpu.VMEM((blocks, HEAD, BLOCK), bf),
            pltpu.VMEM((blocks, HEAD + 8, BLOCK), f32),
            pltpu.VMEM((blocks, 1, BLOCK), f32),
            pltpu.VMEM((BLOCK, BLOCK), f32),
            pltpu.VMEM((BLOCK, BLOCK), f32),
            pltpu.VMEM((own, n * HEAD), bf),
            dma((2 * n, 3)), dma((2 * n, 3)), dma((3,)), dma((16,)), dma((7 * per,)), dma((4, 2)), dma((n,)), dma((16,)),
            dma((pieces,)), dma((n, per)), dma((per,)), dma((14,)), dma((n, 2)), dma, dma((per, 4)),
        ],
        compiler_params=pltpu.CompilerParams(collective_id=0, has_side_effects=True, vmem_limit_bytes=VMEM),
        cost_estimate=pl.CostEstimate(flops=2 * tokens * width * 4 * HEAD + 2 * tokens * tokens * HEAD,
                                      bytes_accessed=2 * tokens * width * 2, transcendentals=tokens * tokens // 2),
    )(x, gain, *tables, wq, wk, wv, wo)
    return moved(y)


def moved(y):
    parts = 4
    rows = y.shape[0] // parts

    def body(y_ref, out_ref, buffer, took, gave):
        def take(i):
            return pltpu.make_async_copy(y_ref.at[pl.ds(i * rows, rows)], buffer.at[i], took.at[i])

        def give(i):
            return pltpu.make_async_copy(buffer.at[i], out_ref.at[pl.ds(i * rows, rows)], gave.at[i])

        for i in range(parts):
            take(i).start()
        for i in range(parts):
            take(i).wait()
            give(i).start()
        for i in range(parts):
            give(i).wait()

    return pl.pallas_call(
        body,
        in_specs=[pl.BlockSpec(memory_space=pl.ANY)],
        out_specs=pl.BlockSpec(memory_space=pl.ANY),
        out_shape=jax.ShapeDtypeStruct(y.shape, y.dtype),
        scratch_shapes=[pltpu.VMEM((parts, rows, y.shape[1]), y.dtype), pltpu.SemaphoreType.DMA((parts,)), pltpu.SemaphoreType.DMA((parts,))],
        compiler_params=pltpu.CompilerParams(vmem_limit_bytes=VMEM),
    )(y)


def tables(tokens):
    speed = float(THETA) ** (-np.arange(HEAD // 2) / (HEAD // 2))
    near, far = np.arange(NEAR)[:, None] * speed, np.arange(0, tokens, NEAR)[:, None] * speed
    return tuple(jnp.asarray(f(t), jnp.float32) for t in (near, far) for f in (np.cos, np.sin))


def solution(mesh):
    n = mesh.shape["sp"]

    def step(x, gain, wq, wk, wv, wo):
        return layer(n, x, gain, tables(n * x.shape[0]), wq, wk, wv, wo)

    tokens, whole = P(("dp", "sp"), None), P("sp", None)
    return jax.shard_map(
        step,
        mesh=mesh,
        in_specs=(tokens, P(None), whole, whole, whole, whole),
        out_specs=tokens,
        check_vma=False,
    )
```

```python
import functools

import jax
import jax.numpy as jnp
import numpy as np
from jax import lax
from jax.experimental import pallas as pl
from jax.experimental.pallas import tpu as pltpu
from jax.sharding import PartitionSpec as P

MESH = pl.DeviceIdType.MESH
HEAD = 256
THETA = 10000
PIECE = 256
BLOCK = 512
STRIP = 256
NEAR = 128
HIDDEN = -2e30
LOG2E = 1.4426950408889634
VMEM = 67043328


def dot(a, b, ca, cb):
    return lax.dot_general(a, b, (((ca,), (cb,)), ((), ())), preferred_element_type=jnp.float32)


def kernel(n, x_ref, gain, cosr, sinr, cosp, sinp, wq, wk, wv, wo, y_ref, wo_all,
           w_s, own_s, land, q_s, k_s, v_s, mix_s, top_s, s0, s1, o_in,
           send_w, recv_w, own_w, send_a, recv_a, recv_f, load_s, send_r, send_o, recv_o, own_o, send_wo, recv_wo, own_wo, out_s):
    s, group = lax.axis_index("sp"), lax.axis_index("dp")
    core, chip = lax.rem(s, 2), lax.div(s, 2)
    chips = n // 2
    sib = s + 1 - 2 * core
    right, left = lax.rem(s + 2, n), lax.rem(s + n - 2, n)
    side = lax.rem(group, 2)
    other = group + 1 - 2 * side
    per = x_ref.shape[0] // PIECE
    depth = wq.shape[0]
    half = depth // 2
    e = HEAD**-0.5 * LOG2E

    def remote(src, dst, ss, rs, to):
        return pltpu.make_async_remote_copy(src_ref=src, dst_ref=dst, send_sem=ss, recv_sem=rs, device_id={"sp": to}, device_id_type=MESH)

    def across(src, dst, ss, rs):
        return pltpu.make_async_remote_copy(src_ref=src, dst_ref=dst, send_sem=ss, recv_sem=rs, device_id={"dp": other}, device_id_type=MESH)

    def load_own(i):
        return pltpu.make_async_copy(x_ref.at[pl.ds(i * PIECE, PIECE)], own_s.at[i], load_s.at[i])

    for i in range(per):
        load_own(i).start()

    barrier = pltpu.get_barrier_semaphore()
    for off in range(1, n):
        pl.semaphore_signal(barrier, inc=1, device_id={"sp": lax.rem(s + off, n)}, device_id_type=MESH)
    pl.semaphore_signal(barrier, inc=1, device_id={"dp": other}, device_id_type=MESH)
    pl.semaphore_wait(barrier, n)

    def rows(d, h):
        return pl.ds(pl.multiple_of(d * depth + h * half, half), half)

    def weight(off, m, frm, to):
        w = (wq, wk, wv)[m]
        return remote(w.at[pl.ds(pl.multiple_of(side * half, half), half), pl.ds(pl.multiple_of(to * HEAD, HEAD), HEAD)],
                      w_s.at[rows(frm, side), pl.ds(m * HEAD, HEAD)], send_w.at[off, m], recv_w.at[off, m], to)

    def hand(off, m, frm, h):
        part = w_s.at[rows(frm, h), pl.ds(m * HEAD, HEAD)]
        return across(part, part, send_w.at[n + off, m], recv_w.at[n + off, m])

    def to_sib(m, frm, to):
        w = (wq, wk, wv)[m]
        return remote(w.at[:, pl.ds(pl.multiple_of(to * HEAD, HEAD), HEAD)],
                      w_s.at[pl.ds(pl.multiple_of(frm * depth, depth), depth), pl.ds(m * HEAD, HEAD)], send_w.at[0, m], recv_w.at[0, m], to)

    away = [4, 5, 2, 6, 3, 7]

    def partner(off, back):
        base = lax.rem(s + (n - (off - off % 2) if back else off - off % 2), n)
        return base + 1 - 2 * core if off % 2 else base

    for off in away:
        for m in range(3):
            weight(off, m, s, partner(off, False)).start()
    for m in range(3):
        to_sib(m, s, sib).start()
    own_weights = [pltpu.make_async_copy(w.at[:, pl.ds(pl.multiple_of(s * HEAD, HEAD), HEAD)],
                                         w_s.at[pl.ds(pl.multiple_of(s * depth, depth), depth), pl.ds(m * HEAD, HEAD)],
                                         own_w.at[m]) for m, w in enumerate((wq, wk, wv))]
    for c in own_weights:
        c.start()
    own_out = pltpu.make_async_copy(wo, wo_all.at[pl.ds(pl.multiple_of(s * depth, depth), depth)], own_wo)
    own_out.start()

    def from_left(b, by):
        return 4 * b + by

    def from_right(b, by):
        return 4 * b + 2 + by

    def from_far(b, by):
        return 16 + 2 * b + by

    def from_sib(i):
        return 24 + i

    def swap(i):
        return remote(own_s.at[i], land.at[from_sib(i)], send_a.at[i], recv_a.at[from_sib(i)], sib)

    def norm(i, rows_at_once=32):
        def some(j, _):
            at = pl.ds(pl.multiple_of(j * rows_at_once, rows_at_once), rows_at_once)
            wide = own_s[i, at, :].astype(jnp.float32)
            scale = lax.rsqrt(jnp.mean(wide * wide, -1, keepdims=True) + 1e-6)
            own_s[i, at, :] = (wide * scale * gain[...].astype(jnp.float32)[None]).astype(jnp.bfloat16)

        lax.fori_loop(0, PIECE // rows_at_once, some, None)

    for i in range(per):
        load_own(i).wait()
        norm(i)
        if i:
            swap(i - 1).start()
    swap(per - 1).start()

    def arrived(slot):
        remote(land.at[slot], land.at[slot], send_a.at[0], recv_a.at[slot], sib).wait_recv()

    for b in range(2):
        arrived(from_sib(2 * b + core))

    def ring(i, b, to, slot):
        mine = core == b // 2

        @pl.when(mine)
        def _():
            remote(own_s.at[2 * (b % 2) + core], land.at[slot], send_r.at[i], recv_a.at[slot], to).start()

        @pl.when(jnp.logical_not(mine))
        def _():
            remote(land.at[from_sib(2 * (b % 2) + core)], land.at[slot], send_r.at[i], recv_a.at[slot], to).start()

    for b in range(4):
        ring(b, b, right, from_left(b, core))
        ring(4 + b, b, left, from_right(b, core))

    for off in away:
        frm = partner(off, True)
        for m in range(3):
            weight(off, m, frm, s).wait_recv()
            hand(off, m, frm, side).start()

    def project(piece, g):
        y = dot(piece, w_s[...], 1, 0)
        cr, sr, turns = cosr[...], sinr[...], []
        for h in range(PIECE // NEAR):
            at = pl.ds(g * (PIECE // NEAR) + h, 1)
            cp, sp = cosp[at, :], sinp[at, :]
            turns.append((cp * cr - sp * sr, sp * cr + cp * sr))
        cos, sin = (jnp.concatenate(t, 0) for t in zip(*turns))
        b, at = lax.div(g, 2), pl.multiple_of(lax.rem(g, 2) * PIECE, PIECE)
        for ref, first in ((q_s, 0), (k_s, HEAD)):
            t = y[:, first : first + HEAD].astype(jnp.bfloat16).astype(jnp.float32)
            lo, hi = t[:, : HEAD // 2], t[:, HEAD // 2 :]
            ref[b, pl.ds(at, PIECE), :] = jnp.concatenate([lo * cos - hi * sin, hi * cos + lo * sin], -1).astype(jnp.bfloat16)
        v_s[b, :, pl.ds(at, PIECE)] = y[:, 2 * HEAD :].astype(jnp.bfloat16).T

    def diagonal(g):
        strips = [((h + 1) * STRIP, slice(h * STRIP, (h + 1) * STRIP)) for h in range(BLOCK // STRIP)]
        found = [dot(k_s[g, :seen, :], q_s[g, cols, :], 1, 1) for seen, cols in strips]
        tops, weights = [], []
        for (seen, cols), t in zip(strips, found):
            ok = lax.broadcasted_iota(jnp.int32, t.shape, 1) + cols.start >= lax.broadcasted_iota(jnp.int32, t.shape, 0)
            t = jnp.where(ok, t, HIDDEN)
            tops.append(t.max(axis=0, keepdims=True))
            weights.append(jnp.exp2((t - tops[-1]) * e).astype(jnp.bfloat16))
        for (seen, cols), top, p in zip(strips, tops, weights):
            top_s[g, :, cols] = top
            mix_s[g, :, cols] = dot(jnp.concatenate([v_s[g, :, :seen], jnp.ones((8, seen), jnp.bfloat16)], 0), p, 1, 0)

    def scores(pair):
        return dot(k_s[pair[1]], q_s[pair[0]], 1, 1)

    def pair_step(now, later, pair, following):
        q, k = pair
        values = jnp.concatenate([v_s[k], jnp.ones((8, BLOCK), jnp.bfloat16)], 0)
        new = scores(following)
        later[...] = new
        olds = top_s[q]
        tops = jnp.maximum(olds, now[...].max(axis=0, keepdims=True))
        top_s[q] = tops
        keeps = jnp.exp2((olds - tops) * e)
        for h in range(BLOCK // STRIP):
            cols = slice(h * STRIP, (h + 1) * STRIP)
            p = jnp.exp2((now[:, cols] - tops[:, cols]) * e).astype(jnp.bfloat16)
            mix_s[q, :, cols] = mix_s[q, :, cols] * keeps[:, cols] + dot(values, p, 1, 0)

    def pairs(count, pick, meanwhile, before=lambda: None):
        s0[...] = scores(pick(jnp.int32(0)))
        before()
        turns = lax.div(count + 1, 2)

        def body(u, _):
            t = 2 * u

            @pl.when(u == jnp.maximum(turns - 5, 0))
            def _():
                meanwhile()

            pair_step(s0, s1, pick(t), pick(jnp.minimum(t + 1, count - 1)))

            @pl.when(t + 1 < count)
            def _():
                pair_step(s1, s0, pick(t + 1), pick(jnp.minimum(t + 2, count - 1)))

        lax.fori_loop(0, turns, body, None)

    first = 4 * chip
    chip_left, chip_right, chip_far = (4 * lax.rem(chip + d, chips) for d in (chips - 1, 1, 2))

    def old(i):
        near = jnp.where(lax.rem(i, 2) == 0, chip_left, chip_right) + lax.div(i - 4, 2)
        return jnp.where(i < 4, first + i, jnp.where(i < 12, near, chip_far + i - 12))

    def relay(i, slot):
        return remote(land.at[slot], land.at[slot], send_a.at[i], recv_a.at[slot], sib)

    def forward(i, slot, b, h, to):
        at = pl.ds(h * (PIECE // 2), PIECE // 2)
        return remote(land.at[slot, at], land.at[from_far(b, core), at], send_r.at[i], recv_f.at[b, h], to)

    def near_come(b):
        for i, slot in enumerate((from_left(b, core), from_right(b, core))):
            arrived(slot)
            relay(4 + 2 * b + i, slot).start()
            forward(8 + 2 * b + i, slot, b, i, (right, left)[i]).start()

    def far_come(b):
        for h in range(2):
            forward(0, jnp.int32(0), b, h, sib).wait_recv()
        relay(12 + b, from_far(b, core)).start()

    for c in own_weights:
        c.wait()
    for m in range(3):
        to_sib(m, sib, s).wait_recv()
    for off in away:
        for m in range(3):
            hand(off, m, partner(off, True), 1 - side).wait_recv()
    lax.fori_loop(0, per, lambda i, _: project(own_s[i], per * s + i), None)
    for b in range(2):
        arrived(from_sib(2 * b + 1 - core))
    lax.fori_loop(0, per, lambda i, _: project(land[from_sib(i)], per * sib + i), None)
    lax.fori_loop(0, 4, lambda b, _: diagonal(first + b), None)

    def pick_own(t):
        q = 1 + (t >= 1).astype(jnp.int32) + (t >= 3).astype(jnp.int32)
        return first + q, first + t - lax.div(q * (q - 1), 2)

    pairs(jnp.int32(6), pick_own, lambda: near_come(jnp.int32(0)))

    def turn(r, _):
        blocks = chip_left + r, chip_right + r

        def go(i, _):
            by = jnp.where(i < 2, core, 1 - core)

            @pl.when(i == 2)
            def _():
                arrived(from_left(r, 1 - core))
                arrived(from_right(r, 1 - core))

            even = lax.rem(i, 2) == 0
            project(land[jnp.where(even, from_left(r, by), from_right(r, by))], 2 * jnp.where(even, blocks[0], blocks[1]) + by)

        lax.fori_loop(0, 4, go, None)
        lax.fori_loop(0, 2, lambda i, _: diagonal(jnp.where(i == 0, blocks[0], blocks[1])), None)

        def pick(t):
            new = jnp.where(lax.rem(t, 2) == 0, blocks[1], blocks[0])
            was = old(lax.div(t, 2))
            return jnp.maximum(new, was), jnp.minimum(new, was)

        def meanwhile():
            @pl.when(r < 3)
            def _():
                near_come(r + 1)

            @pl.when(r == 3)
            def _():
                far_come(jnp.int32(0))

        pairs(9 + 4 * r, pick, meanwhile)

    lax.fori_loop(0, 4, turn, None)

    def out_rows(d, h):
        return wo_all.at[rows(d, h)]

    def out_own(i, h, to):
        return remote(wo.at[pl.ds(pl.multiple_of(h * half, half), half)], out_rows(s, h), send_wo.at[i], recv_wo.at[s, h], to)

    def came(d, h):
        remote(out_rows(d, h), out_rows(d, h), send_wo.at[0], recv_wo.at[d, h], sib).wait_recv()

    def pass_on(i, d, h, to):
        return remote(out_rows(d, h), out_rows(d, h), send_wo.at[i], recv_wo.at[d, h], to)

    def pass_across(i, d):
        return across(out_rows(d, side), out_rows(d, side), send_wo.at[i], recv_wo.at[d, side])

    out_own(0, side, right).start()
    out_own(1, side, left).start()
    out_own(2, jnp.int32(0), sib).start()
    out_own(3, jnp.int32(1), sib).start()

    far = lax.rem(s + 4, n)

    def out_near():
        came(left, side)
        came(right, side)

        @pl.when(core == 0)
        def _():
            pass_on(4, left, side, right).start()

        @pl.when(core == 1)
        def _():
            pass_on(4, right, side, left).start()

        for i, d in enumerate((left, right)):
            pass_across(5 + i, d).start()
            pass_on(7 + i, d, side, sib).start()

    def far_turn(r, _):
        b = chip_far + r

        def go(i, _):
            by = jnp.where(i == 0, core, 1 - core)

            @pl.when(i == 1)
            def _():
                arrived(from_far(r, 1 - core))

            project(land[from_far(r, by)], 2 * b + by)

        lax.fori_loop(0, 2, go, None)

        def pick(t):
            was = old(t)
            return jnp.maximum(b, was), jnp.minimum(b, was)

        def meanwhile():
            @pl.when(r < 3)
            def _():
                far_come(r + 1)

            @pl.when(r == 3)
            def _():
                out_near()

        pairs(12 + r, pick, meanwhile, lambda: diagonal(b))

    lax.fori_loop(0, 4, far_turn, None)

    pieces = n * per

    def dest(i):
        p = lax.rem(i, n)
        p = jnp.where(p < n - 2, lax.rem(p + (n // 2) * (1 - core), n - 2), p)
        on = jnp.where(p < 4, 1 + 2 * lax.rem(p, 2), jnp.where(p < 6, 2, 0))
        flip = jnp.where(p < 4, lax.div(p, 2), jnp.where(p < 6, p - 4, 7 - p))
        to = lax.rem(s + 2 * on, n)
        return to + flip * (1 - 2 * core), lax.div(i, n)

    def target(frm, part):
        return o_in.at[pl.ds(pl.multiple_of(part * PIECE, PIECE), PIECE), pl.ds(pl.multiple_of(frm * HEAD, HEAD), HEAD)]

    def result(g):
        return q_s.at[lax.div(g, 2), pl.ds(pl.multiple_of(lax.rem(g, 2) * PIECE, PIECE), PIECE)]

    def give(i):
        to, part = dest(i)
        return remote(result(per * to + part), target(s, part), send_o.at[i], recv_o.at[s, part], to)

    def keep(part):
        return pltpu.make_async_copy(result(per * s + part), target(s, part), own_o.at[part])

    def send(i):
        @pl.when(lax.rem(i, n) < n - 1)
        def _():
            give(i).start()

        @pl.when(lax.rem(i, n) == n - 1)
        def _():
            keep(lax.div(i, n)).start()

    def finish(i, _):
        to, part = dest(i)
        g = per * to + part
        mix = mix_s[lax.div(g, 2), :, pl.ds(pl.multiple_of(lax.rem(g, 2) * PIECE, PIECE), PIECE)]
        result(g)[...] = (mix[:HEAD] * (1 / mix[HEAD : HEAD + 1])).T.astype(jnp.bfloat16)

        @pl.when(i > 0)
        def _():
            send(i - 1)

    lax.fori_loop(0, pieces, finish, None)

    for i in range(per):
        swap(i).wait_send()
    for i in range(8):
        remote(own_s.at[0], land.at[0], send_r.at[i], recv_a.at[0], sib).wait_send()
    for i in range(per):
        load_own(i).start()
    send(jnp.int32(pieces - 1))

    came(far, side)
    pass_across(9, far).start()
    pass_on(10, far, side, sib).start()
    for i, d in enumerate((left, right, far)):
        came(d, 1 - side)
        pass_on(11 + i, d, 1 - side, sib).start()
    for h in range(2):
        came(sib, jnp.int32(h))
        for d in (left, right, far):
            came(d + 1 - 2 * core, jnp.int32(h))
    own_out.wait()
    for i in range(per):
        load_own(i).wait()

    for i in range(8):
        forward(8 + i, jnp.int32(0), jnp.int32(0), 0, right).wait_send()
    for i in range(4, 16):
        relay(i, jnp.int32(0)).wait_send()

    def load_out(d):
        return pltpu.make_async_copy(wo_all.at[pl.ds(d * depth, depth)], land.at[d], load_s.at[d])

    for d in range(n):
        load_out(d).start()
    for d in range(n):
        load_out(d).wait()

    width = wo_all.shape[1]
    wide = width // 4

    def out(part, j):
        cols = pl.ds(pl.multiple_of(j * wide, wide), wide)
        return pltpu.make_async_copy(land.at[n + part, :, cols], y_ref.at[pl.ds(pl.multiple_of(part * PIECE, PIECE), PIECE), cols],
                                     out_s.at[part, j])

    def last(part, _):
        keep(part).wait()
        for off in range(1, n):
            frm = lax.rem(s + off, n)
            remote(result(jnp.int32(0)), target(frm, part), send_o.at[0], recv_o.at[frm, part], frm).wait_recv()

        def columns(j, _):
            cols = pl.ds(pl.multiple_of(j * wide, wide), wide)
            y = dot(o_in[pl.ds(pl.multiple_of(part * PIECE, PIECE), PIECE), :], land[:n, :, cols].reshape(n * HEAD, wide), 1, 0)
            land[n + part, :, cols] = (own_s[part, :, cols].astype(jnp.float32) + y).astype(jnp.bfloat16)
            out(part, j).start()

        lax.fori_loop(0, width // wide, columns, None)

    lax.fori_loop(0, per, last, None)

    for off in away:
        for m in range(3):
            weight(off, m, s, partner(off, False)).wait_send()
            hand(off, m, partner(off, True), side).wait_send()
    for m in range(3):
        to_sib(m, s, sib).wait_send()
    for i in range(14):
        pass_on(i, jnp.int32(0), jnp.int32(0), sib).wait_send()

    def sent(i, _):
        @pl.when(lax.rem(i, n) < n - 1)
        def _():
            give(i).wait_send()

    lax.fori_loop(0, pieces, sent, None)
    for i in range(per):
        for j in range(width // wide):
            out(jnp.int32(i), jnp.int32(j)).wait()


def layer(n, x, gain, tables, wq, wk, wv, wo):
    own, width = x.shape
    pieces, blocks = n * own // PIECE, n * own // BLOCK
    anywhere, whole = pl.BlockSpec(memory_space=pl.ANY), pl.BlockSpec(memory_space=pltpu.VMEM)
    dma = pltpu.SemaphoreType.DMA
    bf, f32 = jnp.bfloat16, jnp.float32
    tokens, per = n * own, own // PIECE
    y, _ = pl.pallas_call(
        functools.partial(kernel, n),
        in_specs=[anywhere] + [whole] * 5 + [anywhere] * 4,
        out_specs=[anywhere] * 2,
        out_shape=[jax.ShapeDtypeStruct(x.shape, bf), jax.ShapeDtypeStruct((n * HEAD, width), bf)],
        scratch_shapes=[
            pltpu.VMEM((width, 3 * HEAD), bf),
            pltpu.VMEM((per, PIECE, width), bf),
            pltpu.VMEM((7 * per, PIECE, width), bf),
            pltpu.VMEM((blocks, BLOCK, HEAD), bf),
            pltpu.VMEM((blocks, BLOCK, HEAD), bf),
            pltpu.VMEM((blocks, HEAD, BLOCK), bf),
            pltpu.VMEM((blocks, HEAD + 8, BLOCK), f32),
            pltpu.VMEM((blocks, 1, BLOCK), f32),
            pltpu.VMEM((BLOCK, BLOCK), f32),
            pltpu.VMEM((BLOCK, BLOCK), f32),
            pltpu.VMEM((own, n * HEAD), bf),
            dma((2 * n, 3)), dma((2 * n, 3)), dma((3,)), dma((16,)), dma((7 * per,)), dma((4, 2)), dma((n,)), dma((16,)),
            dma((pieces,)), dma((n, per)), dma((per,)), dma((14,)), dma((n, 2)), dma, dma((per, 4)),
        ],
        compiler_params=pltpu.CompilerParams(collective_id=0, has_side_effects=True, vmem_limit_bytes=VMEM),
        cost_estimate=pl.CostEstimate(flops=2 * tokens * width * 4 * HEAD + 2 * tokens * tokens * HEAD,
                                      bytes_accessed=2 * tokens * width * 2, transcendentals=tokens * tokens // 2),
    )(x, gain, *tables, wq, wk, wv, wo)
    return moved(y)


def moved(y):
    parts = 4
    rows = y.shape[0] // parts

    def body(y_ref, out_ref, buffer, took, gave):
        def take(i):
            return pltpu.make_async_copy(y_ref.at[pl.ds(i * rows, rows)], buffer.at[i], took.at[i])

        def give(i):
            return pltpu.make_async_copy(buffer.at[i], out_ref.at[pl.ds(i * rows, rows)], gave.at[i])

        for i in range(parts):
            take(i).start()
        for i in range(parts):
            take(i).wait()
            give(i).start()
        for i in range(parts):
            give(i).wait()

    return pl.pallas_call(
        body,
        in_specs=[pl.BlockSpec(memory_space=pl.ANY)],
        out_specs=pl.BlockSpec(memory_space=pl.ANY),
        out_shape=jax.ShapeDtypeStruct(y.shape, y.dtype),
        scratch_shapes=[pltpu.VMEM((parts, rows, y.shape[1]), y.dtype), pltpu.SemaphoreType.DMA((parts,)), pltpu.SemaphoreType.DMA((parts,))],
        compiler_params=pltpu.CompilerParams(vmem_limit_bytes=VMEM),
    )(y)


def tables(tokens):
    speed = float(THETA) ** (-np.arange(HEAD // 2) / (HEAD // 2))
    near, far = np.arange(NEAR)[:, None] * speed, np.arange(0, tokens, NEAR)[:, None] * speed
    return tuple(jnp.asarray(f(t), jnp.float32) for t in (near, far) for f in (np.cos, np.sin))


def solution(mesh):
    n = mesh.shape["sp"]

    def step(x, gain, wq, wk, wv, wo):
        return layer(n, x, gain, tables(n * x.shape[0]), wq, wk, wv, wo)

    tokens, whole = P(("dp", "sp"), None), P("sp", None)
    return jax.shard_map(
        step,
        mesh=mesh,
        in_specs=(tokens, P(None), whole, whole, whole, whole),
        out_specs=tokens,
        check_vma=False,
    )
```

```python
import functools

import jax
import jax.numpy as jnp
import numpy as np
from jax import lax
from jax.experimental import pallas as pl
from jax.experimental.pallas import tpu as pltpu
from jax.sharding import PartitionSpec as P

MESH = pl.DeviceIdType.MESH
HEAD = 256
THETA = 10000
PIECE = 256
BLOCK = 512
STRIP = 256
NEAR = 128
HIDDEN = -2e30
LOG2E = 1.4426950408889634
VMEM = 67043328


def dot(a, b, ca, cb):
    return lax.dot_general(a, b, (((ca,), (cb,)), ((), ())), preferred_element_type=jnp.float32)


def kernel(n, x_ref, gain, cosr, sinr, cosp, sinp, wq, wk, wv, wo, y_ref, wo_all,
           w_s, own_s, land, q_s, k_s, v_s, mix_s, top_s, s0, s1, o_in,
           send_w, recv_w, own_w, send_a, recv_a, recv_f, load_s, send_r, send_o, recv_o, own_o, send_wo, recv_wo, own_wo, out_s):
    s, group = lax.axis_index("sp"), lax.axis_index("dp")
    core, chip = lax.rem(s, 2), lax.div(s, 2)
    chips = n // 2
    sib = s + 1 - 2 * core
    right, left = lax.rem(s + 2, n), lax.rem(s + n - 2, n)
    side = lax.rem(group, 2)
    other = group + 1 - 2 * side
    per = x_ref.shape[0] // PIECE
    depth = wq.shape[0]
    half = depth // 2
    e = HEAD**-0.5 * LOG2E

    def remote(src, dst, ss, rs, to):
        return pltpu.make_async_remote_copy(src_ref=src, dst_ref=dst, send_sem=ss, recv_sem=rs, device_id={"sp": to}, device_id_type=MESH)

    def across(src, dst, ss, rs):
        return pltpu.make_async_remote_copy(src_ref=src, dst_ref=dst, send_sem=ss, recv_sem=rs, device_id={"dp": other}, device_id_type=MESH)

    def load_own(i):
        return pltpu.make_async_copy(x_ref.at[pl.ds(i * PIECE, PIECE)], own_s.at[i], load_s.at[i])

    for i in range(per):
        load_own(i).start()

    barrier = pltpu.get_barrier_semaphore()
    for off in range(1, n):
        pl.semaphore_signal(barrier, inc=1, device_id={"sp": lax.rem(s + off, n)}, device_id_type=MESH)
    pl.semaphore_signal(barrier, inc=1, device_id={"dp": other}, device_id_type=MESH)
    pl.semaphore_wait(barrier, n)

    def rows(d, h):
        return pl.ds(pl.multiple_of(d * depth + h * half, half), half)

    def weight(off, m, frm, to):
        w = (wq, wk, wv)[m]
        return remote(w.at[pl.ds(pl.multiple_of(side * half, half), half), pl.ds(pl.multiple_of(to * HEAD, HEAD), HEAD)],
                      w_s.at[rows(frm, side), pl.ds(m * HEAD, HEAD)], send_w.at[off, m], recv_w.at[off, m], to)

    def hand(off, m, frm, h):
        part = w_s.at[rows(frm, h), pl.ds(m * HEAD, HEAD)]
        return across(part, part, send_w.at[n + off, m], recv_w.at[n + off, m])

    def to_sib(m, frm, to):
        w = (wq, wk, wv)[m]
        return remote(w.at[:, pl.ds(pl.multiple_of(to * HEAD, HEAD), HEAD)],
                      w_s.at[pl.ds(pl.multiple_of(frm * depth, depth), depth), pl.ds(m * HEAD, HEAD)], send_w.at[0, m], recv_w.at[0, m], to)

    away = [4, 5, 2, 6, 3, 7]

    def partner(off, back):
        base = lax.rem(s + (n - (off - off % 2) if back else off - off % 2), n)
        return base + 1 - 2 * core if off % 2 else base

    for off in away:
        for m in range(3):
            weight(off, m, s, partner(off, False)).start()
    for m in range(3):
        to_sib(m, s, sib).start()
    own_weights = [pltpu.make_async_copy(w.at[:, pl.ds(pl.multiple_of(s * HEAD, HEAD), HEAD)],
                                         w_s.at[pl.ds(pl.multiple_of(s * depth, depth), depth), pl.ds(m * HEAD, HEAD)],
                                         own_w.at[m]) for m, w in enumerate((wq, wk, wv))]
    for c in own_weights:
        c.start()
    own_out = pltpu.make_async_copy(wo, wo_all.at[pl.ds(pl.multiple_of(s * depth, depth), depth)], own_wo)
    own_out.start()

    def from_left(b, by):
        return 4 * b + by

    def from_right(b, by):
        return 4 * b + 2 + by

    def from_far(b, by):
        return 16 + 2 * b + by

    def from_sib(i):
        return 24 + i

    def swap(i):
        return remote(own_s.at[i], land.at[from_sib(i)], send_a.at[i], recv_a.at[from_sib(i)], sib)

    def norm(i, rows_at_once=32):
        def some(j, _):
            at = pl.ds(pl.multiple_of(j * rows_at_once, rows_at_once), rows_at_once)
            wide = own_s[i, at, :].astype(jnp.float32)
            scale = lax.rsqrt(jnp.mean(wide * wide, -1, keepdims=True) + 1e-6)
            own_s[i, at, :] = (wide * scale * gain[...].astype(jnp.float32)[None]).astype(jnp.bfloat16)

        lax.fori_loop(0, PIECE // rows_at_once, some, None)

    for i in range(per):
        load_own(i).wait()
        norm(i)
        if i:
            swap(i - 1).start()
    swap(per - 1).start()

    def arrived(slot):
        remote(land.at[slot], land.at[slot], send_a.at[0], recv_a.at[slot], sib).wait_recv()

    for b in range(2):
        arrived(from_sib(2 * b + core))

    def ring(i, b, to, slot):
        mine = core == b // 2

        @pl.when(mine)
        def _():
            remote(own_s.at[2 * (b % 2) + core], land.at[slot], send_r.at[i], recv_a.at[slot], to).start()

        @pl.when(jnp.logical_not(mine))
        def _():
            remote(land.at[from_sib(2 * (b % 2) + core)], land.at[slot], send_r.at[i], recv_a.at[slot], to).start()

    for b in range(4):
        ring(b, b, right, from_left(b, core))
        ring(4 + b, b, left, from_right(b, core))

    for off in away:
        frm = partner(off, True)
        for m in range(3):
            weight(off, m, frm, s).wait_recv()
            hand(off, m, frm, side).start()

    def project(piece, g):
        y = dot(piece, w_s[...], 1, 0)
        cr, sr, turns = cosr[...], sinr[...], []
        for h in range(PIECE // NEAR):
            at = pl.ds(g * (PIECE // NEAR) + h, 1)
            cp, sp = cosp[at, :], sinp[at, :]
            turns.append((cp * cr - sp * sr, sp * cr + cp * sr))
        cos, sin = (jnp.concatenate(t, 0) for t in zip(*turns))
        b, at = lax.div(g, 2), pl.multiple_of(lax.rem(g, 2) * PIECE, PIECE)
        for ref, first in ((q_s, 0), (k_s, HEAD)):
            t = y[:, first : first + HEAD].astype(jnp.bfloat16).astype(jnp.float32)
            lo, hi = t[:, : HEAD // 2], t[:, HEAD // 2 :]
            ref[b, pl.ds(at, PIECE), :] = jnp.concatenate([lo * cos - hi * sin, hi * cos + lo * sin], -1).astype(jnp.bfloat16)
        v_s[b, :, pl.ds(at, PIECE)] = y[:, 2 * HEAD :].astype(jnp.bfloat16).T

    def diagonal(g):
        strips = [((h + 1) * STRIP, slice(h * STRIP, (h + 1) * STRIP)) for h in range(BLOCK // STRIP)]
        found = [dot(k_s[g, :seen, :], q_s[g, cols, :], 1, 1) for seen, cols in strips]
        tops, weights = [], []
        for (seen, cols), t in zip(strips, found):
            ok = lax.broadcasted_iota(jnp.int32, t.shape, 1) + cols.start >= lax.broadcasted_iota(jnp.int32, t.shape, 0)
            t = jnp.where(ok, t, HIDDEN)
            tops.append(t.max(axis=0, keepdims=True))
            weights.append(jnp.exp2((t - tops[-1]) * e).astype(jnp.bfloat16))
        for (seen, cols), top, p in zip(strips, tops, weights):
            top_s[g, :, cols] = top
            mix_s[g, :, cols] = dot(jnp.concatenate([v_s[g, :, :seen], jnp.ones((8, seen), jnp.bfloat16)], 0), p, 1, 0)

    def scores(pair):
        return dot(k_s[pair[1]], q_s[pair[0]], 1, 1)

    def pair_step(now, later, pair, following):
        q, k = pair
        values = jnp.concatenate([v_s[k], jnp.ones((8, BLOCK), jnp.bfloat16)], 0)
        new = scores(following)
        later[...] = new
        olds = top_s[q]
        tops = jnp.maximum(olds, now[...].max(axis=0, keepdims=True))
        top_s[q] = tops
        keeps = jnp.exp2((olds - tops) * e)
        for h in range(BLOCK // STRIP):
            cols = slice(h * STRIP, (h + 1) * STRIP)
            p = jnp.exp2((now[:, cols] - tops[:, cols]) * e).astype(jnp.bfloat16)
            mix_s[q, :, cols] = mix_s[q, :, cols] * keeps[:, cols] + dot(values, p, 1, 0)

    def pairs(count, pick, meanwhile, before=lambda: None):
        s0[...] = scores(pick(jnp.int32(0)))
        before()
        turns = lax.div(count + 1, 2)

        def body(u, _):
            t = 2 * u

            @pl.when(u == jnp.maximum(turns - 6, 0))
            def _():
                meanwhile()

            pair_step(s0, s1, pick(t), pick(jnp.minimum(t + 1, count - 1)))

            @pl.when(t + 1 < count)
            def _():
                pair_step(s1, s0, pick(t + 1), pick(jnp.minimum(t + 2, count - 1)))

        lax.fori_loop(0, turns, body, None)

    first = 4 * chip
    chip_left, chip_right, chip_far = (4 * lax.rem(chip + d, chips) for d in (chips - 1, 1, 2))

    def old(i):
        near = jnp.where(lax.rem(i, 2) == 0, chip_left, chip_right) + lax.div(i - 4, 2)
        return jnp.where(i < 4, first + i, jnp.where(i < 12, near, chip_far + i - 12))

    def relay(i, slot):
        return remote(land.at[slot], land.at[slot], send_a.at[i], recv_a.at[slot], sib)

    def forward(i, slot, b, h, to):
        at = pl.ds(h * (PIECE // 2), PIECE // 2)
        return remote(land.at[slot, at], land.at[from_far(b, core), at], send_r.at[i], recv_f.at[b, h], to)

    def near_come(b):
        for i, slot in enumerate((from_left(b, core), from_right(b, core))):
            arrived(slot)
            relay(4 + 2 * b + i, slot).start()
            forward(8 + 2 * b + i, slot, b, i, (right, left)[i]).start()

    def far_come(b):
        for h in range(2):
            forward(0, jnp.int32(0), b, h, sib).wait_recv()
        relay(12 + b, from_far(b, core)).start()

    for c in own_weights:
        c.wait()
    for m in range(3):
        to_sib(m, sib, s).wait_recv()
    for off in away:
        for m in range(3):
            hand(off, m, partner(off, True), 1 - side).wait_recv()
    lax.fori_loop(0, per, lambda i, _: project(own_s[i], per * s + i), None)
    for b in range(2):
        arrived(from_sib(2 * b + 1 - core))
    lax.fori_loop(0, per, lambda i, _: project(land[from_sib(i)], per * sib + i), None)
    lax.fori_loop(0, 4, lambda b, _: diagonal(first + b), None)

    def pick_own(t):
        q = 1 + (t >= 1).astype(jnp.int32) + (t >= 3).astype(jnp.int32)
        return first + q, first + t - lax.div(q * (q - 1), 2)

    pairs(jnp.int32(6), pick_own, lambda: near_come(jnp.int32(0)))

    def turn(r, _):
        blocks = chip_left + r, chip_right + r

        def go(i, _):
            by = jnp.where(i < 2, core, 1 - core)

            @pl.when(i == 2)
            def _():
                arrived(from_left(r, 1 - core))
                arrived(from_right(r, 1 - core))

            even = lax.rem(i, 2) == 0
            project(land[jnp.where(even, from_left(r, by), from_right(r, by))], 2 * jnp.where(even, blocks[0], blocks[1]) + by)

        lax.fori_loop(0, 4, go, None)
        lax.fori_loop(0, 2, lambda i, _: diagonal(jnp.where(i == 0, blocks[0], blocks[1])), None)

        def pick(t):
            new = jnp.where(lax.rem(t, 2) == 0, blocks[1], blocks[0])
            was = old(lax.div(t, 2))
            return jnp.maximum(new, was), jnp.minimum(new, was)

        def meanwhile():
            @pl.when(r < 3)
            def _():
                near_come(r + 1)

            @pl.when(r == 3)
            def _():
                far_come(jnp.int32(0))

        pairs(9 + 4 * r, pick, meanwhile)

    lax.fori_loop(0, 4, turn, None)

    def out_rows(d, h):
        return wo_all.at[rows(d, h)]

    def out_own(i, h, to):
        return remote(wo.at[pl.ds(pl.multiple_of(h * half, half), half)], out_rows(s, h), send_wo.at[i], recv_wo.at[s, h], to)

    def came(d, h):
        remote(out_rows(d, h), out_rows(d, h), send_wo.at[0], recv_wo.at[d, h], sib).wait_recv()

    def pass_on(i, d, h, to):
        return remote(out_rows(d, h), out_rows(d, h), send_wo.at[i], recv_wo.at[d, h], to)

    def pass_across(i, d):
        return across(out_rows(d, side), out_rows(d, side), send_wo.at[i], recv_wo.at[d, side])

    out_own(0, side, right).start()
    out_own(1, side, left).start()
    out_own(2, jnp.int32(0), sib).start()
    out_own(3, jnp.int32(1), sib).start()

    far = lax.rem(s + 4, n)

    def out_near():
        came(left, side)
        came(right, side)

        @pl.when(core == 0)
        def _():
            pass_on(4, left, side, right).start()

        @pl.when(core == 1)
        def _():
            pass_on(4, right, side, left).start()

        for i, d in enumerate((left, right)):
            pass_across(5 + i, d).start()
            pass_on(7 + i, d, side, sib).start()

    def far_turn(r, _):
        b = chip_far + r

        def go(i, _):
            by = jnp.where(i == 0, core, 1 - core)

            @pl.when(i == 1)
            def _():
                arrived(from_far(r, 1 - core))

            project(land[from_far(r, by)], 2 * b + by)

        lax.fori_loop(0, 2, go, None)

        def pick(t):
            was = old(t)
            return jnp.maximum(b, was), jnp.minimum(b, was)

        def meanwhile():
            @pl.when(r < 3)
            def _():
                far_come(r + 1)

            @pl.when(r == 3)
            def _():
                out_near()

        pairs(12 + r, pick, meanwhile, lambda: diagonal(b))

    lax.fori_loop(0, 4, far_turn, None)

    pieces = n * per

    def dest(i):
        p = lax.rem(i, n)
        p = jnp.where(p < n - 2, lax.rem(p + (n // 2) * (1 - core), n - 2), p)
        on = jnp.where(p < 4, 1 + 2 * lax.rem(p, 2), jnp.where(p < 6, 2, 0))
        flip = jnp.where(p < 4, lax.div(p, 2), jnp.where(p < 6, p - 4, 7 - p))
        to = lax.rem(s + 2 * on, n)
        return to + flip * (1 - 2 * core), lax.div(i, n)

    def target(frm, part):
        return o_in.at[pl.ds(pl.multiple_of(part * PIECE, PIECE), PIECE), pl.ds(pl.multiple_of(frm * HEAD, HEAD), HEAD)]

    def result(g):
        return q_s.at[lax.div(g, 2), pl.ds(pl.multiple_of(lax.rem(g, 2) * PIECE, PIECE), PIECE)]

    def give(i):
        to, part = dest(i)
        return remote(result(per * to + part), target(s, part), send_o.at[i], recv_o.at[s, part], to)

    def keep(part):
        return pltpu.make_async_copy(result(per * s + part), target(s, part), own_o.at[part])

    def send(i):
        @pl.when(lax.rem(i, n) < n - 1)
        def _():
            give(i).start()

        @pl.when(lax.rem(i, n) == n - 1)
        def _():
            keep(lax.div(i, n)).start()

    def finish(i, _):
        to, part = dest(i)
        g = per * to + part
        mix = mix_s[lax.div(g, 2), :, pl.ds(pl.multiple_of(lax.rem(g, 2) * PIECE, PIECE), PIECE)]
        result(g)[...] = (mix[:HEAD] * (1 / mix[HEAD : HEAD + 1])).T.astype(jnp.bfloat16)

        @pl.when(i > 0)
        def _():
            send(i - 1)

    lax.fori_loop(0, pieces, finish, None)

    for i in range(per):
        swap(i).wait_send()
    for i in range(8):
        remote(own_s.at[0], land.at[0], send_r.at[i], recv_a.at[0], sib).wait_send()
    for i in range(per):
        load_own(i).start()
    send(jnp.int32(pieces - 1))

    came(far, side)
    pass_across(9, far).start()
    pass_on(10, far, side, sib).start()
    for i, d in enumerate((left, right, far)):
        came(d, 1 - side)
        pass_on(11 + i, d, 1 - side, sib).start()
    for h in range(2):
        came(sib, jnp.int32(h))
        for d in (left, right, far):
            came(d + 1 - 2 * core, jnp.int32(h))
    own_out.wait()
    for i in range(per):
        load_own(i).wait()

    for i in range(8):
        forward(8 + i, jnp.int32(0), jnp.int32(0), 0, right).wait_send()
    for i in range(4, 16):
        relay(i, jnp.int32(0)).wait_send()

    def load_out(d):
        return pltpu.make_async_copy(wo_all.at[pl.ds(d * depth, depth)], land.at[d], load_s.at[d])

    for d in range(n):
        load_out(d).start()
    for d in range(n):
        load_out(d).wait()

    width = wo_all.shape[1]
    wide = width // 4

    def out(part, j):
        cols = pl.ds(pl.multiple_of(j * wide, wide), wide)
        return pltpu.make_async_copy(land.at[n + part, :, cols], y_ref.at[pl.ds(pl.multiple_of(part * PIECE, PIECE), PIECE), cols],
                                     out_s.at[part, j])

    def last(part, _):
        keep(part).wait()
        for off in range(1, n):
            frm = lax.rem(s + off, n)
            remote(result(jnp.int32(0)), target(frm, part), send_o.at[0], recv_o.at[frm, part], frm).wait_recv()

        def columns(j, _):
            cols = pl.ds(pl.multiple_of(j * wide, wide), wide)
            y = dot(o_in[pl.ds(pl.multiple_of(part * PIECE, PIECE), PIECE), :], land[:n, :, cols].reshape(n * HEAD, wide), 1, 0)
            land[n + part, :, cols] = (own_s[part, :, cols].astype(jnp.float32) + y).astype(jnp.bfloat16)
            out(part, j).start()

        lax.fori_loop(0, width // wide, columns, None)

    lax.fori_loop(0, per, last, None)

    for off in away:
        for m in range(3):
            weight(off, m, s, partner(off, False)).wait_send()
            hand(off, m, partner(off, True), side).wait_send()
    for m in range(3):
        to_sib(m, s, sib).wait_send()
    for i in range(14):
        pass_on(i, jnp.int32(0), jnp.int32(0), sib).wait_send()

    def sent(i, _):
        @pl.when(lax.rem(i, n) < n - 1)
        def _():
            give(i).wait_send()

    lax.fori_loop(0, pieces, sent, None)
    for i in range(per):
        for j in range(width // wide):
            out(jnp.int32(i), jnp.int32(j)).wait()


def layer(n, x, gain, tables, wq, wk, wv, wo):
    own, width = x.shape
    pieces, blocks = n * own // PIECE, n * own // BLOCK
    anywhere, whole = pl.BlockSpec(memory_space=pl.ANY), pl.BlockSpec(memory_space=pltpu.VMEM)
    dma = pltpu.SemaphoreType.DMA
    bf, f32 = jnp.bfloat16, jnp.float32
    tokens, per = n * own, own // PIECE
    y, _ = pl.pallas_call(
        functools.partial(kernel, n),
        in_specs=[anywhere] + [whole] * 5 + [anywhere] * 4,
        out_specs=[anywhere] * 2,
        out_shape=[jax.ShapeDtypeStruct(x.shape, bf), jax.ShapeDtypeStruct((n * HEAD, width), bf)],
        scratch_shapes=[
            pltpu.VMEM((width, 3 * HEAD), bf),
            pltpu.VMEM((per, PIECE, width), bf),
            pltpu.VMEM((7 * per, PIECE, width), bf),
            pltpu.VMEM((blocks, BLOCK, HEAD), bf),
            pltpu.VMEM((blocks, BLOCK, HEAD), bf),
            pltpu.VMEM((blocks, HEAD, BLOCK), bf),
            pltpu.VMEM((blocks, HEAD + 8, BLOCK), f32),
            pltpu.VMEM((blocks, 1, BLOCK), f32),
            pltpu.VMEM((BLOCK, BLOCK), f32),
            pltpu.VMEM((BLOCK, BLOCK), f32),
            pltpu.VMEM((own, n * HEAD), bf),
            dma((2 * n, 3)), dma((2 * n, 3)), dma((3,)), dma((16,)), dma((7 * per,)), dma((4, 2)), dma((n,)), dma((16,)),
            dma((pieces,)), dma((n, per)), dma((per,)), dma((14,)), dma((n, 2)), dma, dma((per, 4)),
        ],
        compiler_params=pltpu.CompilerParams(collective_id=0, has_side_effects=True, vmem_limit_bytes=VMEM),
        cost_estimate=pl.CostEstimate(flops=2 * tokens * width * 4 * HEAD + 2 * tokens * tokens * HEAD,
                                      bytes_accessed=2 * tokens * width * 2, transcendentals=tokens * tokens // 2),
    )(x, gain, *tables, wq, wk, wv, wo)
    return moved(y)


def moved(y):
    parts = 4
    rows = y.shape[0] // parts

    def body(y_ref, out_ref, buffer, took, gave):
        def take(i):
            return pltpu.make_async_copy(y_ref.at[pl.ds(i * rows, rows)], buffer.at[i], took.at[i])

        def give(i):
            return pltpu.make_async_copy(buffer.at[i], out_ref.at[pl.ds(i * rows, rows)], gave.at[i])

        for i in range(parts):
            take(i).start()
        for i in range(parts):
            take(i).wait()
            give(i).start()
        for i in range(parts):
            give(i).wait()

    return pl.pallas_call(
        body,
        in_specs=[pl.BlockSpec(memory_space=pl.ANY)],
        out_specs=pl.BlockSpec(memory_space=pl.ANY),
        out_shape=jax.ShapeDtypeStruct(y.shape, y.dtype),
        scratch_shapes=[pltpu.VMEM((parts, rows, y.shape[1]), y.dtype), pltpu.SemaphoreType.DMA((parts,)), pltpu.SemaphoreType.DMA((parts,))],
        compiler_params=pltpu.CompilerParams(vmem_limit_bytes=VMEM),
    )(y)


def tables(tokens):
    speed = float(THETA) ** (-np.arange(HEAD // 2) / (HEAD // 2))
    near, far = np.arange(NEAR)[:, None] * speed, np.arange(0, tokens, NEAR)[:, None] * speed
    return tuple(jnp.asarray(f(t), jnp.float32) for t in (near, far) for f in (np.cos, np.sin))


def solution(mesh):
    n = mesh.shape["sp"]

    def step(x, gain, wq, wk, wv, wo):
        return layer(n, x, gain, tables(n * x.shape[0]), wq, wk, wv, wo)

    tokens, whole = P(("dp", "sp"), None), P("sp", None)
    return jax.shard_map(
        step,
        mesh=mesh,
        in_specs=(tokens, P(None), whole, whole, whole, whole),
        out_specs=tokens,
        check_vma=False,
    )
```
